32 devices in a mesh: data: 1 (over z), col: 4 (over y), row: 8 (over x, core).
Axes of the slice: x: 4, y: 4, z: 1, core: 2. Of those that a mesh axis runs over, the one named last changes fastest.
The devices are a block of a 4x4x8 slice.
Arguments:
- pair_rep: bfloat16 [512, 512, 64], P(('data', 'row'), 'col')
- res_mask: int32 [512], P('data')
- ln_gamma: float32 [64], replicated
- ln_beta: float32 [64], replicated
- w_q: bfloat16 [64, 64], replicated
- w_k: bfloat16 [64, 64], replicated
- w_v: bfloat16 [64, 64], replicated
- w_b: bfloat16 [64, 4], replicated
- w_g: bfloat16 [64, 64], replicated
- w_o: bfloat16 [64, 64], replicated
Outputs:
- output: bfloat16 [512, 512, 64], P(('data', 'row'), 'col')
All inputs are finite; a program needn't handle non-finite values.
Results may differ from the reference program's by a relative error of at most 0.00619686.
Values are sent between devices in bfloat16 or wider.
A program may use at most 768 MiB of HBM per device.

```python
import math
import jax
import jax.numpy as jnp
from jax import lax

N = 512
C_Z = 64
HEADS = 4
HEAD = 16

PROJ = HEADS * HEAD
Q_SCALE = 1.0 / math.sqrt(HEAD)
LN_EPS = 1e-5
MASK_FILL = -1e9
OUT_GAIN = 0.35 * math.sqrt(N / PROJ)


def setup_inputs(seed: int = 0, part: int = 0) -> dict:
    base_key = jax.random.key(seed)
    part_key = jax.random.fold_in(base_key, part)
    key_pair, key_len = jax.random.split(part_key, 2)
    pair_rep = jax.random.normal(key_pair, (N, N, C_Z), jnp.float32).astype(jnp.bfloat16)
    pad_len = jax.random.randint(key_len, (), N // 16, N // 4 + 1)
    res_mask = (jnp.arange(N) < N - pad_len).astype(jnp.int32)
    weight_keys = jax.random.split(base_key, 8)
    in_scale = 1.0 / math.sqrt(C_Z)
    ln_gamma = jax.random.uniform(weight_keys[0], (C_Z,), jnp.float32, 0.5, 1.5)
    ln_beta = 0.1 * jax.random.normal(weight_keys[1], (C_Z,), jnp.float32)
    w_q = (in_scale * jax.random.normal(weight_keys[2], (C_Z, PROJ), jnp.float32)).astype(jnp.bfloat16)
    w_k = (in_scale * jax.random.normal(weight_keys[3], (C_Z, PROJ), jnp.float32)).astype(jnp.bfloat16)
    w_v = (in_scale * jax.random.normal(weight_keys[4], (C_Z, PROJ), jnp.float32)).astype(jnp.bfloat16)
    w_b = (in_scale * jax.random.normal(weight_keys[5], (C_Z, HEADS), jnp.float32)).astype(jnp.bfloat16)
    w_g = (in_scale * jax.random.normal(weight_keys[6], (C_Z, PROJ), jnp.float32)).astype(jnp.bfloat16)
    w_o = (OUT_GAIN * jax.random.normal(weight_keys[7], (PROJ, C_Z), jnp.float32)).astype(jnp.bfloat16)
    return {'pair_rep': pair_rep, 'res_mask': res_mask, 'ln_gamma': ln_gamma, 'ln_beta': ln_beta, 'w_q': w_q, 'w_k': w_k, 'w_v': w_v, 'w_b': w_b, 'w_g': w_g, 'w_o': w_o}


def reference(pair_rep, res_mask, ln_gamma, ln_beta, w_q, w_k, w_v, w_b, w_g, w_o):
    pair_f32 = pair_rep.astype(jnp.float32)
    mean = jnp.mean(pair_f32, axis=-1, keepdims=True)
    centred = pair_f32 - mean
    variance = jnp.mean(centred * centred, axis=-1, keepdims=True)
    normed = (centred * lax.rsqrt(variance + LN_EPS) * ln_gamma + ln_beta).astype(jnp.bfloat16)
    bias = jnp.dot(normed.reshape(N * N, C_Z), w_b, preferred_element_type=jnp.float32).astype(jnp.bfloat16).reshape(N, N, HEADS)
    key_fill = jnp.where(res_mask > 0, 0.0, MASK_FILL).astype(jnp.float32)
    bias_ik = jnp.transpose(bias, (1, 0, 2)).astype(jnp.float32) + key_fill[None, :, None]

    def one_column(col_args):
        a_col, z_col = col_args
        query = (jnp.dot(a_col, w_q, preferred_element_type=jnp.float32) * Q_SCALE).astype(jnp.bfloat16).reshape(N, HEADS, HEAD)
        keys = jnp.dot(a_col, w_k, preferred_element_type=jnp.float32).astype(jnp.bfloat16).reshape(N, HEADS, HEAD)
        values = jnp.dot(a_col, w_v, preferred_element_type=jnp.float32).astype(jnp.bfloat16).reshape(N, HEADS, HEAD)
        gate = jax.nn.sigmoid(jnp.dot(a_col, w_g, preferred_element_type=jnp.float32))
        logits = jnp.einsum('ihd,khd->ikh', query.astype(jnp.float32), keys.astype(jnp.float32)) + bias_ik
        attn_prob = jax.nn.softmax(logits, axis=1)
        attended = jnp.einsum('ikh,khd->ihd', attn_prob, values.astype(jnp.float32)).reshape(N, PROJ)
        gated = (gate * attended).astype(jnp.bfloat16)
        return (z_col.astype(jnp.float32) + jnp.dot(gated, w_o, preferred_element_type=jnp.float32)).astype(jnp.bfloat16)

    out_cols = lax.map(one_column, (jnp.transpose(normed, (1, 0, 2)), jnp.transpose(pair_rep, (1, 0, 2))))
    return jnp.transpose(out_cols, (1, 0, 2))
```

```python
import functools
import math

import jax
import jax.numpy as jnp
from jax import lax
from jax.experimental import pallas as pl
from jax.experimental.pallas import tpu as pltpu
from jax.sharding import PartitionSpec as P

LN_EPS = 1e-5
MASK_FILL = -1e9
MESH = pl.DeviceIdType.MESH
F32, BF16 = jnp.float32, jnp.bfloat16
NT = (((1,), (1,)), ((), ()))
PAD = 8


def mm(a, b):
    return jnp.dot(a, b, preferred_element_type=F32)


def mm_nt(a, b):
    return lax.dot_general(a, b, NT, preferred_element_type=F32)


def tr(w):
    return jnp.transpose(w.astype(F32)).astype(BF16)


def block_diag2(w):
    z = jnp.zeros_like(w)
    return jnp.concatenate([jnp.concatenate([w, z], 1), jnp.concatenate([z, w], 1)], 0)


def remote(src, dst, send, recv, dev):
    return pltpu.make_async_remote_copy(src_ref=src, dst_ref=dst, send_sem=send, recv_sem=recv, device_id=dev, device_id_type=MESH)


def gather_kernel(rows, cols, z_ref, gamma_ref, beta_ref, wb_ref, a_ref, bias_ref, stage, bsc, send, a_sem, x_sem, y_sem, f_sem):
    ti, ch, tj = z_ref.shape
    heads = wb_ref.shape[0]
    cj = tj // rows
    hj = cj // 2
    pitch = rows * hj + PAD
    me_r, me_c = lax.axis_index('row'), lax.axis_index('col')
    core = me_r % 2
    partner = me_r + 1 - 2 * core

    barrier = pltpu.get_barrier_semaphore()
    for d in range(1, rows):
        pl.semaphore_signal(barrier, inc=1, device_id={'row': (me_r + d) % rows}, device_id_type=MESH)
    for d in range(1, cols):
        pl.semaphore_signal(barrier, inc=1, device_id={'col': (me_c + d) % cols}, device_id_type=MESH)

    gam = jnp.transpose(jnp.broadcast_to(gamma_ref[...], (tj, ch)))
    bet = jnp.transpose(jnp.broadcast_to(beta_ref[...], (tj, ch)))
    group = 4
    wb = wb_ref[...].astype(F32)
    wb16 = jnp.concatenate([wb] * group, 0)
    wb16 = jnp.concatenate([wb16] * group, 1)
    r_id = lax.broadcasted_iota(jnp.int32, wb16.shape, 0) // heads
    c_id = lax.broadcasted_iota(jnp.int32, wb16.shape, 1) // ch
    wb16 = jnp.where(r_id == c_id, wb16, 0.0).astype(BF16)

    def norm_step(t, _):
        x = z_ref[pl.ds(t * group, group)].astype(F32)
        mean = jnp.sum(x, axis=1, keepdims=True) * (1.0 / ch)
        cen = x - mean
        var = jnp.sum(cen * cen, axis=1, keepdims=True) * (1.0 / ch)
        n = cen * lax.rsqrt(var + LN_EPS) * gam + bet
        nb = n.astype(BF16)
        bsc[pl.ds(pl.multiple_of(t * group * heads, group * heads), group * heads), :] = mm(wb16, nb.reshape(group * ch, tj))
        for q in range(group):
            t4 = jnp.transpose(n[q]).reshape(rows, 2, hj, ch)
            packed = jnp.concatenate([t4[:, 0], t4[:, 1]], axis=-1).reshape(rows * hj, 2 * ch)
            stage[pl.ds(pl.multiple_of((t * group + q) * pitch, 8), rows * hj), :] = packed
        return 0

    lax.fori_loop(0, ti // group, norm_step, 0)

    my_rows = pl.ds(pl.multiple_of(me_r * ti, ti), ti)
    for h in range(heads):
        bias_ref[me_c, h, my_rows, :] = bsc[pl.ds(h, ti, stride=heads), :].astype(BF16)

    pl.semaphore_wait(barrier, rows + cols - 2)

    def x_copy(d, src_row):
        rs = pl.ds(pl.multiple_of(src_row * ti, ti), ti)
        return remote(bias_ref.at[me_c, :, rs, :], bias_ref.at[me_c, :, rs, :], x_sem.at[0, d], x_sem.at[1, d], {'row': (me_r + d) % rows})

    def a_copy(d, dst_row, src_row):
        rs = pl.ds(pl.multiple_of(src_row * ti, ti), ti)
        return remote(send.at[dst_row], a_ref.at[:, rs, :], a_sem.at[0, d], a_sem.at[1, d], {'row': (me_r + d) % rows})

    def piece(dst_row, jp):
        return stage[pl.ds(dst_row * hj + jp, ti, stride=pitch), :].astype(BF16)

    order = [4, 3, 5, 2, 6, 1, 7] if rows == 8 else list(range(1, rows))
    for d in order:
        x_copy(d, me_r).start()
    last = None
    for d in order:
        dst = (me_r + d) % rows
        for jp in range(hj):
            send[dst, jp] = piece(dst, jp)
        if last is not None:
            last.start()
        last = a_copy(d, dst, me_r)
    for jp in range(hj):
        a_ref[jp, my_rows, :] = piece(me_r, jp)
    last.start()

    hh = heads // 2
    mine, other = pl.ds(core * hh, hh), pl.ds((1 - core) * hh, hh)

    def y_copy(d, blk):
        return remote(bias_ref.at[blk, mine], bias_ref.at[blk, mine], y_sem.at[0, d], y_sem.at[1, d], {'col': (me_c + d) % cols})

    def f_copy(d, blk, part):
        return remote(bias_ref.at[blk, part], bias_ref.at[blk, part], f_sem.at[0, d], f_sem.at[1, d], {'row': partner})

    for d in order:
        x_copy(d, (me_r + rows - d) % rows).wait_recv()
    y_order = [2, 1, 3] if cols == 4 else list(range(1, cols))
    for d in y_order:
        y_copy(d, me_c).start()
    for d in y_order:
        blk = (me_c + cols - d) % cols
        y_copy(d, blk).wait_recv()
        f_copy(d, blk, mine).start()
    for d in y_order:
        f_copy(d, (me_c + cols - d) % cols, other).wait_recv()
    for d in order:
        a_copy(d, me_r, (me_r + rows - d) % rows).wait_recv()
    for d in order:
        x_copy(d, me_r).wait_send()
        a_copy(d, (me_r + d) % rows, me_r).wait_send()
    for d in y_order:
        y_copy(d, me_c).wait_send()
        f_copy(d, me_c, mine).wait_send()


def attend_kernel(a_ref, bias_ref, mask_ref, wq_ref, wk_ref, wv_ref, wg_ref, out_ref, qt, vt, gt, kk, bf, ga):
    hj, n, two_ch = a_ref.shape
    cols, heads, _, tj = bias_ref.shape
    ch = two_ch // 2
    e = wq_ref.shape[1] // heads
    proj = heads * e

    w3 = jnp.concatenate([tr(wq_ref[...]), tr(wv_ref[...]), tr(wg_ref[...])], 0)
    w6 = block_diag2(w3)
    wk2 = block_diag2(wk_ref[...])
    q_scale = 1.0 / math.sqrt(e)

    fill = jnp.where(mask_ref[...] > 0, 0.0, MASK_FILL).astype(F32)
    fill_col = jnp.transpose(jnp.broadcast_to(fill, (tj, n)))

    def bias_step(t, _):
        bf[t] = bias_ref[t // heads, t % heads].astype(F32) + fill_col
        return 0

    lax.fori_loop(0, cols * heads, bias_step, 0)

    def proj_step(jp, _):
        a = a_ref[jp]
        r = mm_nt(w6, a)
        for half in range(2):
            o = half * 3 * proj
            dst = pl.ds(half * proj, proj)
            q = (r[o:o + proj] * q_scale).astype(BF16)
            g = jax.nn.sigmoid(r[o + 2 * proj:o + 3 * proj])
            vt[jp, dst, :] = r[o + proj:o + 2 * proj].astype(BF16)
            for ib in range(cols):
                qt[jp, ib, dst, :] = q[:, ib * tj:(ib + 1) * tj]
                gt[jp, ib, dst, :] = g[:, ib * tj:(ib + 1) * tj]
        kk[jp] = mm(a, wk2).astype(BF16)
        return 0

    lax.fori_loop(0, hj, proj_step, 0)

    def unit(t, _):
        ib, jp = t // hj, t % hj
        for h in range(heads):
            z16 = jnp.zeros((e, tj), BF16)
            rhs = []
            for half in range(2):
                for hh in range(heads):
                    if hh == h:
                        qv = qt[jp, ib, half * proj + h * e:half * proj + (h + 1) * e, :]
                        pair = [qv, z16] if half == 0 else [z16, qv]
                        rhs.append(jnp.concatenate(pair, 1))
                    else:
                        rhs.append(jnp.zeros((e, 2 * tj), BF16))
            rhs = jnp.concatenate(rhs, 0)
            bb = bf[ib * heads + h]
            s = mm(kk[jp], rhs) + jnp.concatenate([bb, bb], 1)
            m = jnp.max(s, axis=0, keepdims=True)
            p = jnp.exp(s - m)
            l = jnp.sum(p, axis=0, keepdims=True)
            v2 = jnp.concatenate([vt[jp, h * e:(h + 1) * e, :], vt[jp, proj + h * e:proj + (h + 1) * e, :]], 0)
            o = mm(v2, p.astype(BF16))
            for half in range(2):
                lanes = slice(half * tj, (half + 1) * tj)
                rs = slice(half * proj + h * e, half * proj + (h + 1) * e)
                ga[rs, :] = gt[jp, ib, rs, :] * (o[half * e:(half + 1) * e, lanes] / l[:, lanes])
        out_ref[jp, pl.ds(pl.multiple_of(ib * tj, tj), tj), :] = jnp.transpose(ga[...]).astype(BF16)
        return 0

    lax.fori_loop(0, cols * hj, unit, 0)


def return_kernel(rows, g_ref, out_ref, sem):
    hj, n, lanes = g_ref.shape
    ti = n // rows
    me_r = lax.axis_index('row')
    barrier = pltpu.get_barrier_semaphore()
    for d in range(1, rows):
        pl.semaphore_signal(barrier, inc=1, device_id={'row': (me_r + d) % rows}, device_id_type=MESH)
    pl.semaphore_wait(barrier, rows - 1)

    def copy(d, dst_row, slot):
        rs = pl.ds(pl.multiple_of(dst_row * ti, ti), ti)
        return remote(g_ref.at[:, rs, :], out_ref.at[slot], sem.at[0, d], sem.at[1, d], {'row': (me_r + d) % rows})

    order = [4, 3, 5, 2, 6, 1, 7] if rows == 8 else list(range(1, rows))
    for d in order:
        copy(d, (me_r + d) % rows, me_r).start()
    out_ref[me_r] = g_ref[:, pl.ds(pl.multiple_of(me_r * ti, ti), ti), :]
    for d in order:
        copy(d, me_r, (me_r + rows - d) % rows).wait_recv()
    for d in order:
        copy(d, (me_r + d) % rows, me_r).wait_send()


def finish_kernel(g_ref, z_ref, wo_ref, out_ref, stage):
    rows, hj, ti, lanes = g_ref.shape
    ch, tj = z_ref.shape[1:]
    pitch = ti + PAD
    n_rj = rows * hj
    wo = tr(wo_ref[...])
    wo = jnp.concatenate([wo, jnp.zeros_like(wo)], 1)

    def widen(t, _):
        for jp in range(hj):
            stage[pl.ds(pl.multiple_of((t * hj + jp) * pitch, 8), ti), :] = g_ref[t, jp].astype(F32)
        return 0

    lax.fori_loop(0, rows, widen, 0)

    group = 4

    def step(t, _):
        for q in range(group):
            i = t * group + q
            x = stage[pl.ds(i, n_rj, stride=pitch), :]
            y = pltpu.roll(x, ch, 1)
            x2 = jnp.concatenate([x.reshape(rows, 1, hj, lanes), y.reshape(rows, 1, hj, lanes)], 1).reshape(tj, lanes).astype(BF16)
            out_ref[i] = (mm_nt(wo, x2) + z_ref[i].astype(F32)).astype(BF16)
        return 0

    lax.fori_loop(0, ti // group, step, 0)


VM = pl.BlockSpec(memory_space=pltpu.VMEM)


def solution(mesh):
    rows, cols = mesh.shape['row'], mesh.shape['col']

    def body(pair_tile, res_mask, ln_gamma, ln_beta, w_q, w_k, w_v, w_b, w_g, w_o):
        ti, tj, ch = pair_tile.shape
        heads = w_b.shape[1]
        proj = w_q.shape[1]
        n = ti * rows
        hj = tj // rows // 2
        z = jnp.transpose(pair_tile, (0, 2, 1))
        dma = pltpu.SemaphoreType.DMA
        a_cols, bias = pl.pallas_call(
            functools.partial(gather_kernel, rows, cols),
            out_shape=(jax.ShapeDtypeStruct((hj, n, 2 * ch), BF16), jax.ShapeDtypeStruct((cols, heads, n, tj), BF16)),
            in_specs=[VM] * 4,
            out_specs=(VM, VM),
            scratch_shapes=[
                pltpu.VMEM((ti * (rows * hj + PAD), 2 * ch), F32),
                pltpu.VMEM((ti * heads, tj), F32),
                pltpu.VMEM((rows, hj, ti, 2 * ch), BF16),
                dma((2, rows)), dma((2, rows)), dma((2, cols)), dma((2, cols)),
            ],
            compiler_params=pltpu.CompilerParams(collective_id=0, has_side_effects=True),
            name='gather',
        )(z, ln_gamma.reshape(1, ch), ln_beta.reshape(1, ch), w_b.T)
        gated = pl.pallas_call(
            attend_kernel,
            out_shape=jax.ShapeDtypeStruct((hj, n, 2 * ch), BF16),
            in_specs=[VM] * 7,
            out_specs=VM,
            scratch_shapes=[
                pltpu.VMEM((hj, cols, 2 * proj, tj), BF16),
                pltpu.VMEM((hj, 2 * proj, n), BF16),
                pltpu.VMEM((hj, cols, 2 * proj, tj), F32),
                pltpu.VMEM((hj, n, 2 * proj), BF16),
                pltpu.VMEM((cols * heads, n, tj), F32),
                pltpu.VMEM((2 * proj, tj), F32),
            ],
            name='attend',
        )(a_cols, bias, res_mask.reshape(1, n), w_q, w_k, w_v, w_g)
        back = pl.pallas_call(
            functools.partial(return_kernel, rows),
            out_shape=jax.ShapeDtypeStruct((rows, hj, ti, 2 * ch), BF16),
            in_specs=[VM],
            out_specs=VM,
            scratch_shapes=[dma((2, rows))],
            compiler_params=pltpu.CompilerParams(collective_id=1, has_side_effects=True),
            name='back',
        )(gated)
        out = pl.pallas_call(
            finish_kernel,
            out_shape=jax.ShapeDtypeStruct((ti, ch, tj), BF16),
            in_specs=[VM] * 3,
            out_specs=VM,
            scratch_shapes=[pltpu.VMEM((rows * hj * (ti + PAD), 2 * ch), F32)],
            name='finish',
        )(back, z, w_o)
        return jnp.transpose(out, (0, 2, 1))

    tile_spec = P(('data', 'row'), 'col', None)
    return jax.shard_map(body, mesh=mesh, in_specs=(tile_spec, P('data'), P(), P(), P(), P(), P(), P(), P(), P()), out_specs=tile_spec, check_vma=False)
```

```python
import functools
import math

import jax
import jax.numpy as jnp
import numpy as np
from jax import lax
from jax.experimental import pallas as pl
from jax.experimental.pallas import tpu as pltpu
from jax.sharding import PartitionSpec as P

LN_EPS = 1e-5
MASK_FILL = -1e9
MESH = pl.DeviceIdType.MESH
F32, BF16 = jnp.float32, jnp.bfloat16
NT = (((1,), (1,)), ((), ()))
PAD = 8


def mm(a, b):
    return jnp.dot(a, b, preferred_element_type=F32)


def mm_nt(a, b):
    return lax.dot_general(a, b, NT, preferred_element_type=F32)


def tr(w):
    return jnp.transpose(w.astype(F32)).astype(BF16)


def block_diag2(w):
    z = jnp.zeros_like(w)
    return jnp.concatenate([jnp.concatenate([w, z], 1), jnp.concatenate([z, w], 1)], 0)


def remote(src, dst, send, recv, dev):
    return pltpu.make_async_remote_copy(src_ref=src, dst_ref=dst, send_sem=send, recv_sem=recv, device_id=dev, device_id_type=MESH)


def fill_terms():
    rest, terms = MASK_FILL, []
    for _ in range(3):
        t = float(np.asarray(rest, dtype=BF16))
        terms.append(t)
        rest -= t
    return terms


def pair_rows(wt, e):
    z = jnp.zeros_like(wt)
    lo, hi = jnp.concatenate([wt, z], 1), jnp.concatenate([z, wt], 1)
    return [blk for r in range(0, wt.shape[0], e) for blk in (lo[r:r + e], hi[r:r + e])]


def triangle_kernel(rows, cols, z_ref, gamma_ref, beta_ref, wb_ref, mask_ref, wq_ref, wk_ref, wv_ref, wg_ref, out_ref,
                    stage, bsc, send, a_ref, bias_ref, qp, vt, gt, kh, ss, mm_s, ga, outb, a_sem, x_sem, y_sem, f_sem, o_sem):
    ti, ch, tj = z_ref.shape
    heads = wb_ref.shape[0]
    hj, n, lanes = a_ref.shape
    e = wq_ref.shape[1] // heads
    e2 = 2 * e
    proj2 = 2 * heads * e
    q_scale = 1.0 / math.sqrt(e)
    pitch = rows * hj + PAD
    per_blk = tj // ti
    me_r, me_c = lax.axis_index('row'), lax.axis_index('col')
    core = me_r % 2
    partner = me_r + 1 - 2 * core
    chip = me_r // 2

    barrier = pltpu.get_barrier_semaphore()
    for d in range(1, rows):
        pl.semaphore_signal(barrier, inc=1, device_id={'row': (me_r + d) % rows}, device_id_type=MESH)
    for d in range(1, cols):
        pl.semaphore_signal(barrier, inc=1, device_id={'col': (me_c + d) % cols}, device_id_type=MESH)

    gam = jnp.transpose(jnp.broadcast_to(gamma_ref[...], (tj, ch)))
    bet = jnp.transpose(jnp.broadcast_to(beta_ref[...], (tj, ch)))
    group = 4
    wb = wb_ref[...].astype(F32)
    wb16 = jnp.concatenate([wb] * group, 0)
    wb16 = jnp.concatenate([wb16] * group, 1)
    r_id = lax.broadcasted_iota(jnp.int32, wb16.shape, 0) // heads
    c_id = lax.broadcasted_iota(jnp.int32, wb16.shape, 1) // ch
    wb16 = jnp.where(r_id == c_id, wb16, 0.0).astype(BF16)
    unroll = 2

    def norm_step(t, _):
        for u in range(unroll):
            i0 = (t * unroll + u) * group
            x = z_ref[pl.ds(i0, group)].astype(F32)
            mean = jnp.sum(x, axis=1, keepdims=True) * (1.0 / ch)
            cen = x - mean
            var = jnp.sum(cen * cen, axis=1, keepdims=True) * (1.0 / ch)
            nrm = cen * lax.rsqrt(var + LN_EPS) * gam + bet
            bsc[pl.ds(pl.multiple_of(i0 * heads, group * heads), group * heads), :] = mm(wb16, nrm.astype(BF16).reshape(group * ch, tj))
            for q in range(group):
                t4 = jnp.transpose(nrm[q]).reshape(rows, 2, hj, ch)
                packed = jnp.concatenate([t4[:, 0], t4[:, 1]], axis=-1).reshape(rows * hj, 2 * ch)
                stage[pl.ds(pl.multiple_of((i0 + q) * pitch, 8), rows * hj), :] = packed
        return 0

    lax.fori_loop(0, ti // group // unroll, norm_step, 0)

    my_rows = pl.ds(pl.multiple_of(me_r * ti, ti), ti)
    for h in range(heads):
        bias_ref[me_c, h, my_rows, :] = bsc[pl.ds(h, ti, stride=heads), :].astype(BF16)

    def x_copy(d, src_row):
        rs = pl.ds(pl.multiple_of(src_row * ti, ti), ti)
        return remote(bias_ref.at[me_c, :, rs, :], bias_ref.at[me_c, :, rs, :], x_sem.at[0, d], x_sem.at[1, d], {'row': (me_r + d) % rows})

    def a_copy(d, dst_row, src_row):
        rs = pl.ds(pl.multiple_of(src_row * ti, ti), ti)
        return remote(send.at[dst_row], a_ref.at[:, rs, :], a_sem.at[0, d], a_sem.at[1, d], {'row': (me_r + d) % rows})

    def piece(dst_row, jp):
        return stage[pl.ds(dst_row * hj + jp, ti, stride=pitch), :].astype(BF16)

    hh = heads // 2
    mine, other = pl.ds(core * hh, hh), pl.ds((1 - core) * hh, hh)

    def y_copy(d, blk):
        return remote(bias_ref.at[blk, mine], bias_ref.at[blk, mine], y_sem.at[0, d], y_sem.at[1, d], {'col': (me_c + d) % cols})

    def f_copy(d, blk, part):
        return remote(bias_ref.at[blk, part], bias_ref.at[blk, part], f_sem.at[0, d], f_sem.at[1, d], {'row': partner})

    order = [4, 3, 5, 2, 6, 1, 7] if rows == 8 else list(range(1, rows))
    y_order = [2, 1, 3] if cols == 4 else list(range(1, cols))

    pl.semaphore_wait(barrier, rows + cols - 2)
    for d in order:
        x_copy(d, me_r).start()
    last = None
    for d in order:
        dst = (me_r + d) % rows
        for jp in range(hj):
            send[dst, jp] = piece(dst, jp)
        if last is not None:
            last.start()
        last = a_copy(d, dst, me_r)
    for jp in range(hj):
        a_ref[jp, my_rows, :] = piece(me_r, jp)
    last.start()

    w_qvg = jnp.concatenate(pair_rows(tr(wq_ref[...]), e) + pair_rows(tr(wv_ref[...]), e) + pair_rows(tr(wg_ref[...]), e), 0)
    k_rows = pair_rows(tr(wk_ref[...]), e)
    k_pad = jnp.zeros((lanes - e2, lanes), BF16)
    w_kh = jnp.concatenate([b for h in range(heads) for b in (k_rows[2 * h], k_rows[2 * h + 1], k_pad)], 0)
    masked = jnp.broadcast_to(mask_ref[...] == 0, (lanes, n))
    lane_row = lax.broadcasted_iota(jnp.int32, (lanes, n), 0)
    fill = jnp.zeros((lanes, n), F32)
    for t, f in enumerate(fill_terms()):
        fill = jnp.where(masked & (lane_row == e2 + t), f, fill)
    fill_col = jnp.transpose(fill)
    row_id = lax.broadcasted_iota(jnp.int32, (e, 2 * tj), 0)
    ones_rows = jnp.where(row_id < 3, 1.0, 0.0).astype(BF16)
    eye_r = lax.broadcasted_iota(jnp.int32, (tj, 2 * tj), 0)
    eye_c = lax.broadcasted_iota(jnp.int32, (tj, 2 * tj), 1)
    eye2 = jnp.where(eye_r == lax.rem(eye_c, tj), 1.0, 0.0).astype(BF16)
    z16 = jnp.zeros((e, tj), BF16)
    z_rows = jnp.zeros((lanes - 3 * e, 2 * tj), BF16)

    for d in order:
        x_copy(d, (me_r + rows - d) % rows).wait_recv()
    for d in y_order:
        y_copy(d, me_c).start()
    for d in order:
        a_copy(d, me_r, (me_r + rows - d) % rows).wait_recv()

    def proj_step(jp, _):
        a = a_ref[jp]
        r = mm_nt(w_qvg, a)
        q = (r[:proj2] * q_scale).astype(BF16)
        g = jax.nn.sigmoid(r[2 * proj2:])
        vt[jp] = r[proj2:2 * proj2].astype(BF16)
        for ib in range(cols):
            ls = slice(ib * tj, (ib + 1) * tj)
            gt[jp, ib] = g[:, ls]
            for h in range(heads):
                qp[jp, ib, h, 0:e, 0:tj] = q[h * e2:h * e2 + e, ls]
                qp[jp, ib, h, 0:e, tj:2 * tj] = z16
                qp[jp, ib, h, e:e2, 0:tj] = z16
                qp[jp, ib, h, e:e2, tj:2 * tj] = q[h * e2 + e:h * e2 + e2, ls]
                qp[jp, ib, h, e2:3 * e, :] = ones_rows
        k = mm_nt(a, w_kh)
        for h in range(heads):
            kh[jp, h] = (k[:, h * lanes:(h + 1) * lanes] + fill_col).astype(BF16)
        return 0

    lax.fori_loop(0, hj, proj_step, 0)

    away = [2, 1, 3, 0] if cols == 4 else [(k + 1) % cols for k in range(cols)]
    shift = (me_c - chip + cols) % cols
    pos = sum(jnp.where(shift == a, k, 0) for k, a in enumerate(away))

    def block_of(phase):
        k = jnp.where(phase <= pos, phase - 1, phase)
        step = sum(jnp.where(k == i, a, 0) for i, a in enumerate(away))
        return jnp.where(phase == 0, me_c, (chip + step) % cols)

    halves = 2
    ck = n // halves

    def scores_steps(ib, jp, h, slot):
        rhs = jnp.concatenate([qp[jp, ib, h], z_rows, eye2], 0)
        mx = jnp.full((8, 2 * tj), -jnp.inf, F32)
        for c in range(halves):
            rs = slice(c * ck, (c + 1) * ck)
            s = mm(jnp.concatenate([kh[jp, h, rs], bias_ref[ib, h, rs]], 1), rhs)
            ss[slot, rs] = s
            mx = jnp.maximum(mx, jnp.max(s.reshape(ck // 8, 8, 2 * tj), axis=0))
            if c == halves - 1:
                mm_s[slot] = jnp.max(mx, axis=0, keepdims=True)
            yield

    def softmax_steps(ib, jp, h, slot):
        l = jnp.zeros((8, 2 * tj), F32)
        m = mm_s[slot]
        o = jnp.zeros((e2, 2 * tj), F32)
        for c in range(halves):
            rs = slice(c * ck, (c + 1) * ck)
            p = jnp.exp(ss[slot, rs] - m)
            l = l + jnp.sum(p.reshape(ck // 8, 8, 2 * tj), axis=0)
            o = o + mm(vt[jp, h * e2:(h + 1) * e2, rs], p.astype(BF16))
            if c == halves - 1:
                l1 = jnp.sum(l, axis=0, keepdims=True)
                for half in range(2):
                    ls = slice(half * tj, (half + 1) * tj)
                    r2 = slice(h * e2 + half * e, h * e2 + (half + 1) * e)
                    ga[r2, :] = gt[jp, ib, r2, :] * (o[half * e:(half + 1) * e, ls] / l1[:, ls])
            yield

    def out_copy(dst_row, src_jp, slot, slot_jp):
        rs = pl.ds(pl.multiple_of(dst_row * ti, ti), ti)
        return remote(outb.at[src_jp, rs, :], out_ref.at[slot, slot_jp], o_sem.at[0, dst_row], o_sem.at[1, slot], {'row': dst_row})

    def send_out(t):
        ib, jp = block_of(t // hj), t % hj
        for k in range(per_blk):
            dst_row = ib * per_blk + k

            @pl.when(dst_row != me_r)
            def _():
                out_copy(dst_row, jp, me_r, jp).start()

            @pl.when(dst_row == me_r)
            def _():
                out_ref[me_r, jp] = outb[jp, my_rows, :]

    for _ in scores_steps(block_of(0), 0, 0, 0):
        pass

    units = cols * hj

    def unit(t, _):
        for phase in range(1, cols):
            @pl.when(t == phase * hj - 4)
            def _():
                blk = block_of(phase)
                d = (me_c - blk + cols) % cols
                y_copy(d, blk).wait_recv()
                f_copy(d, blk, mine).start()

            @pl.when(t == phase * hj - 1)
            def _():
                blk = block_of(phase)
                d = (me_c - blk + cols) % cols
                f_copy(d, blk, other).wait_recv()

        @pl.when(t > 0)
        def _():
            send_out(t - 1)

        ib, jp = block_of(t // hj), t % hj
        t_next = (t + 1) % units
        ib_next, jp_next = block_of(t_next // hj), t_next % hj
        for h in range(heads):
            nxt = (ib, jp, h + 1) if h + 1 < heads else (ib_next, jp_next, 0)
            for _ in zip(scores_steps(*nxt, (h + 1) % 2), softmax_steps(ib, jp, h, h % 2)):
                pass
        outb[jp, pl.ds(pl.multiple_of(ib * tj, tj), tj), :] = jnp.transpose(ga[...]).astype(BF16)
        return 0

    lax.fori_loop(0, units, unit, 0)
    send_out(units - 1)

    for d in order:
        x_copy(d, me_r).wait_send()
        a_copy(d, (me_r + d) % rows, me_r).wait_send()
    for d in y_order:
        y_copy(d, me_c).wait_send()
        f_copy(d, me_c, mine).wait_send()

    def all_out(send_row, slot):
        rs = pl.ds(pl.multiple_of(send_row * ti, ti), ti)
        return remote(outb.at[:, rs, :], out_ref.at[slot], o_sem.at[0, send_row], o_sem.at[1, slot], {'row': partner})

    for d in order:
        src = (me_r + rows - d) % rows
        all_out(src, src).wait_recv()
    for d in order:
        dst = (me_r + d) % rows
        all_out(dst, dst).wait_send()


def finish_kernel(e, g_ref, z_ref, wo_ref, out_ref, stage):
    rows, hj, ti, lanes = g_ref.shape
    ch, tj = z_ref.shape[1:]
    pitch = ti + PAD
    n_rj = rows * hj
    wo = wo_ref[...].astype(F32)
    z = jnp.zeros((e, ch), F32)
    wo = tr(jnp.concatenate([blk for r in range(0, wo.shape[0], e) for blk in (wo[r:r + e], z)], 0))

    def widen(t, _):
        for jp in range(hj):
            stage[pl.ds(pl.multiple_of((t * hj + jp) * pitch, 8), ti), :] = g_ref[t, jp].astype(F32)
        return 0

    lax.fori_loop(0, rows, widen, 0)

    group = 8

    def step(t, _):
        for q in range(group):
            i = t * group + q
            x = stage[pl.ds(i, n_rj, stride=pitch), :]
            y = pltpu.roll(x, lanes - e, 1)
            x2 = jnp.concatenate([x.reshape(rows, 1, hj, lanes), y.reshape(rows, 1, hj, lanes)], 1).reshape(tj, lanes).astype(BF16)
            out_ref[i] = (mm_nt(wo, x2) + z_ref[i].astype(F32)).astype(BF16)
        return 0

    lax.fori_loop(0, ti // group, step, 0)


VM = pl.BlockSpec(memory_space=pltpu.VMEM)


def solution(mesh):
    rows, cols = mesh.shape['row'], mesh.shape['col']

    def body(pair_tile, res_mask, ln_gamma, ln_beta, w_q, w_k, w_v, w_b, w_g, w_o):
        ti, tj, ch = pair_tile.shape
        heads = w_b.shape[1]
        proj = w_q.shape[1]
        n = ti * rows
        hj = tj // rows // 2
        z = jnp.transpose(pair_tile, (0, 2, 1))
        dma = pltpu.SemaphoreType.DMA
        e = proj // heads
        back = pl.pallas_call(
            functools.partial(triangle_kernel, rows, cols),
            out_shape=jax.ShapeDtypeStruct((rows, hj, ti, 2 * ch), BF16),
            in_specs=[VM] * 9,
            out_specs=VM,
            scratch_shapes=[
                pltpu.VMEM((ti * (rows * hj + PAD), 2 * ch), F32),
                pltpu.VMEM((ti * heads, tj), F32),
                pltpu.VMEM((rows, hj, ti, 2 * ch), BF16),
                pltpu.VMEM((hj, n, 2 * ch), BF16),
                pltpu.VMEM((cols, heads, n, tj), BF16),
                pltpu.VMEM((hj, cols, heads, 3 * e, 2 * tj), BF16),
                pltpu.VMEM((hj, 2 * proj, n), BF16),
                pltpu.VMEM((hj, cols, 2 * proj, tj), F32),
                pltpu.VMEM((hj, heads, n, 2 * ch), BF16),
                pltpu.VMEM((2, n, 2 * tj), F32),
                pltpu.VMEM((2, 1, 2 * tj), F32),
                pltpu.VMEM((2 * proj, tj), F32),
                pltpu.VMEM((hj, n, 2 * proj), BF16),
                dma((2, rows)), dma((2, rows)), dma((2, cols)), dma((2, cols)), dma((2, rows)),
            ],
            compiler_params=pltpu.CompilerParams(collective_id=0, has_side_effects=True),
            name='triangle',
        )(z, ln_gamma.reshape(1, ch), ln_beta.reshape(1, ch), w_b.T, res_mask.reshape(1, n), w_q, w_k, w_v, w_g)
        out = pl.pallas_call(
            functools.partial(finish_kernel, proj // heads),
            out_shape=jax.ShapeDtypeStruct((ti, ch, tj), BF16),
            in_specs=[VM] * 3,
            out_specs=VM,
            scratch_shapes=[pltpu.VMEM((rows * hj * (ti + PAD), 2 * ch), F32)],
            name='finish',
        )(back, z, w_o)
        return jnp.transpose(out, (0, 2, 1))

    tile_spec = P(('data', 'row'), 'col', None)
    return jax.shard_map(body, mesh=mesh, in_specs=(tile_spec, P('data'), P(), P(), P(), P(), P(), P(), P(), P()), out_specs=tile_spec, check_vma=False)
```

```python
import functools
import math

import jax
import jax.numpy as jnp
import numpy as np
from jax import lax
from jax.experimental import pallas as pl
from jax.experimental.pallas import tpu as pltpu
from jax.sharding import PartitionSpec as P

LN_EPS = 1e-5
MASK_FILL = -1e9
MESH = pl.DeviceIdType.MESH
F32, BF16 = jnp.float32, jnp.bfloat16
NT = (((1,), (1,)), ((), ()))
PAD = 8


def mm(a, b):
    return jnp.dot(a, b, preferred_element_type=F32)


def mm_nt(a, b):
    return lax.dot_general(a, b, NT, preferred_element_type=F32)


def tr(w):
    return jnp.transpose(w.astype(F32)).astype(BF16)


def block_diag2(w):
    z = jnp.zeros_like(w)
    return jnp.concatenate([jnp.concatenate([w, z], 1), jnp.concatenate([z, w], 1)], 0)


def remote(src, dst, send, recv, dev):
    return pltpu.make_async_remote_copy(src_ref=src, dst_ref=dst, send_sem=send, recv_sem=recv, device_id=dev, device_id_type=MESH)


def fill_terms():
    rest, terms = MASK_FILL, []
    for _ in range(3):
        t = float(np.asarray(rest, dtype=BF16))
        terms.append(t)
        rest -= t
    return terms


def pair_rows(wt, e):
    z = jnp.zeros_like(wt)
    lo, hi = jnp.concatenate([wt, z], 1), jnp.concatenate([z, wt], 1)
    return [blk for r in range(0, wt.shape[0], e) for blk in (lo[r:r + e], hi[r:r + e])]


def triangle_kernel(rows, cols, z_ref, gamma_ref, beta_ref, wb_ref, mask_ref, wq_ref, wk_ref, wv_ref, wg_ref, out_ref,
                    stage, bsc, bown, send, a_ref, bias_ref, qp, vt, gt, kh, ss, mm_s, ga, outb, a_sem, x_sem, y_sem, f_sem, o_sem):
    ti, ch, tj = z_ref.shape
    heads = wb_ref.shape[0]
    hj, n, lanes = a_ref.shape
    e = wq_ref.shape[1] // heads
    e2 = 2 * e
    proj2 = 2 * heads * e
    q_scale = 1.0 / math.sqrt(e)
    pitch = rows * hj + PAD
    per_blk = tj // ti
    me_r, me_c = lax.axis_index('row'), lax.axis_index('col')
    core = me_r % 2
    partner = me_r + 1 - 2 * core
    chip = me_r // 2

    barrier = pltpu.get_barrier_semaphore()
    for d in range(1, rows):
        pl.semaphore_signal(barrier, inc=1, device_id={'row': (me_r + d) % rows}, device_id_type=MESH)
    for d in range(1, cols):
        pl.semaphore_signal(barrier, inc=1, device_id={'col': (me_c + d) % cols}, device_id_type=MESH)

    gam = jnp.transpose(jnp.broadcast_to(gamma_ref[...], (tj, ch)))
    bet = jnp.transpose(jnp.broadcast_to(beta_ref[...], (tj, ch)))
    group = 4
    wb = wb_ref[...].astype(F32)
    wb16 = jnp.concatenate([wb] * group, 0)
    wb16 = jnp.concatenate([wb16] * group, 1)
    r_id = lax.broadcasted_iota(jnp.int32, wb16.shape, 0) // heads
    c_id = lax.broadcasted_iota(jnp.int32, wb16.shape, 1) // ch
    wb16 = jnp.where(r_id == c_id, wb16, 0.0).astype(BF16)
    unroll = 2

    def norm_step(t, _):
        for u in range(unroll):
            i0 = (t * unroll + u) * group
            x = z_ref[pl.ds(i0, group)].astype(F32)
            mean = jnp.sum(x, axis=1, keepdims=True) * (1.0 / ch)
            cen = x - mean
            var = jnp.sum(cen * cen, axis=1, keepdims=True) * (1.0 / ch)
            nrm = cen * lax.rsqrt(var + LN_EPS) * gam + bet
            bsc[pl.ds(pl.multiple_of(i0 * heads, group * heads), group * heads), :] = mm(wb16, nrm.astype(BF16).reshape(group * ch, tj))
            for q in range(group):
                t4 = jnp.transpose(nrm[q]).reshape(rows, 2, hj, ch)
                packed = jnp.concatenate([t4[:, 0], t4[:, 1]], axis=-1).reshape(rows * hj, 2 * ch)
                stage[pl.ds(pl.multiple_of((i0 + q) * pitch, 8), rows * hj), :] = packed
        return 0

    lax.fori_loop(0, ti // group // unroll, norm_step, 0)

    my_rows = pl.ds(pl.multiple_of(me_r * ti, ti), ti)
    hh = heads // 2
    mine, other = pl.ds(core * hh, hh), pl.ds((1 - core) * hh, hh)
    for h in range(heads):
        bown[h] = bsc[pl.ds(h, ti, stride=heads), :].astype(BF16)
    bias_ref[me_c, mine, my_rows, :] = bown[mine]

    def x_copy(d, dst_row, src_row):
        rs = pl.ds(pl.multiple_of(src_row * ti, ti), ti)
        part = pl.ds((dst_row % 2) * hh, hh)
        return remote(bown.at[part], bias_ref.at[me_c, part, rs, :], x_sem.at[0, d], x_sem.at[1, d], {'row': (me_r + d) % rows})

    def a_copy(d, jp, dst_row, src_row):
        rs = pl.ds(pl.multiple_of(src_row * ti, ti), ti)
        return remote(send.at[dst_row, jp], a_ref.at[jp, rs, :], a_sem.at[0, jp, d], a_sem.at[1, jp, d], {'row': (me_r + d) % rows})

    def piece(dst_row, jp):
        return stage[pl.ds(dst_row * hj + jp, ti, stride=pitch), :].astype(BF16)

    def y_copy(d, blk):
        return remote(bias_ref.at[blk, mine], bias_ref.at[blk, mine], y_sem.at[0, d], y_sem.at[1, d], {'col': (me_c + d) % cols})

    def f_copy(d, blk, part):
        return remote(bias_ref.at[blk, part], bias_ref.at[blk, part], f_sem.at[0, d], f_sem.at[1, d], {'row': partner})

    order = [4, 3, 5, 2, 6, 1, 7] if rows == 8 else list(range(1, rows))
    y_order = [2, 1, 3] if cols == 4 else list(range(1, cols))

    pl.semaphore_wait(barrier, rows + cols - 2)
    for d in order:
        x_copy(d, (me_r + d) % rows, me_r).start()
    for jp in range(hj + 1):
        if jp < hj:
            for d in order:
                dst = (me_r + d) % rows
                send[dst, jp] = piece(dst, jp)
            a_ref[jp, my_rows, :] = piece(me_r, jp)
        if jp > 0:
            for d in order:
                a_copy(d, jp - 1, (me_r + d) % rows, me_r).start()

    w_qvg = jnp.concatenate(pair_rows(tr(wq_ref[...]), e) + pair_rows(tr(wv_ref[...]), e) + pair_rows(tr(wg_ref[...]), e), 0)
    k_rows = pair_rows(tr(wk_ref[...]), e)
    k_pad = jnp.zeros((lanes - e2, lanes), BF16)
    w_kh = jnp.concatenate([b for h in range(heads) for b in (k_rows[2 * h], k_rows[2 * h + 1], k_pad)], 0)
    masked = jnp.broadcast_to(mask_ref[...] == 0, (lanes, n))
    lane_row = lax.broadcasted_iota(jnp.int32, (lanes, n), 0)
    fill = jnp.zeros((lanes, n), F32)
    for t, f in enumerate(fill_terms()):
        fill = jnp.where(masked & (lane_row == e2 + t), f, fill)
    fill_col = jnp.transpose(fill)
    row_id = lax.broadcasted_iota(jnp.int32, (e, 2 * tj), 0)
    ones_rows = jnp.where(row_id < 3, 1.0, 0.0).astype(BF16)
    eye_r = lax.broadcasted_iota(jnp.int32, (tj, 2 * tj), 0)
    eye_c = lax.broadcasted_iota(jnp.int32, (tj, 2 * tj), 1)
    eye2 = jnp.where(eye_r == lax.rem(eye_c, tj), 1.0, 0.0).astype(BF16)
    z16 = jnp.zeros((e, tj), BF16)
    z_rows = jnp.zeros((lanes - 3 * e, 2 * tj), BF16)

    for d in order:
        x_copy(d, me_r, (me_r + rows - d) % rows).wait_recv()
    f_copy(0, me_c, mine).start()
    for d in y_order:
        y_copy(d, me_c).start()

    def wait_cols(jp):
        for d in order:
            a_copy(d, jp, me_r, (me_r + rows - d) % rows).wait_recv()

    def project(jp):
        a = a_ref[jp]
        r = mm_nt(w_qvg, a)
        q = (r[:proj2] * q_scale).astype(BF16)
        g = jax.nn.sigmoid(r[2 * proj2:])
        vt[jp] = r[proj2:2 * proj2].astype(BF16)
        for ib in range(cols):
            ls = slice(ib * tj, (ib + 1) * tj)
            gt[jp, ib] = g[:, ls]
            for h in range(heads):
                qp[jp, ib, h, 0:e, 0:tj] = q[h * e2:h * e2 + e, ls]
                qp[jp, ib, h, 0:e, tj:2 * tj] = z16
                qp[jp, ib, h, e:e2, 0:tj] = z16
                qp[jp, ib, h, e:e2, tj:2 * tj] = q[h * e2 + e:h * e2 + e2, ls]
                qp[jp, ib, h, e2:3 * e, :] = ones_rows
        k = mm_nt(a, w_kh)
        for h in range(heads):
            kh[jp, h] = (k[:, h * lanes:(h + 1) * lanes] + fill_col).astype(BF16)

    away = [2, 1, 3, 0] if cols == 4 else [(k + 1) % cols for k in range(cols)]
    shift = (me_c - chip + cols) % cols
    pos = sum(jnp.where(shift == a, k, 0) for k, a in enumerate(away))

    def block_of(phase):
        k = jnp.where(phase <= pos, phase - 1, phase)
        step = sum(jnp.where(k == i, a, 0) for i, a in enumerate(away))
        return jnp.where(phase == 0, me_c, (chip + step) % cols)

    halves = 2
    ck = n // halves

    def scores_steps(ib, jp, h, slot):
        rhs = jnp.concatenate([qp[jp, ib, h], z_rows, eye2], 0)
        mx = jnp.full((8, 2 * tj), -jnp.inf, F32)
        for c in range(halves):
            rs = slice(c * ck, (c + 1) * ck)
            s = mm(jnp.concatenate([kh[jp, h, rs], bias_ref[ib, h, rs]], 1), rhs)
            ss[slot, rs] = s
            mx = jnp.maximum(mx, jnp.max(s.reshape(ck // 8, 8, 2 * tj), axis=0))
            if c == halves - 1:
                mm_s[slot] = jnp.max(mx, axis=0, keepdims=True)
            yield

    def softmax_steps(ib, jp, h, slot):
        l = jnp.zeros((8, 2 * tj), F32)
        m = mm_s[slot]
        o = jnp.zeros((e2, 2 * tj), F32)
        for c in range(halves):
            rs = slice(c * ck, (c + 1) * ck)
            p = jnp.exp(ss[slot, rs] - m)
            l = l + jnp.sum(p.reshape(ck // 8, 8, 2 * tj), axis=0)
            o = o + mm(vt[jp, h * e2:(h + 1) * e2, rs], p.astype(BF16))
            if c == halves - 1:
                l1 = jnp.sum(l, axis=0, keepdims=True)
                for half in range(2):
                    ls = slice(half * tj, (half + 1) * tj)
                    r2 = slice(h * e2 + half * e, h * e2 + (half + 1) * e)
                    ga[r2, :] = gt[jp, ib, r2, :] * (o[half * e:(half + 1) * e, ls] / l1[:, ls])
            yield

    def out_copy(dst_row, src_jp, slot, slot_jp):
        rs = pl.ds(pl.multiple_of(dst_row * ti, ti), ti)
        return remote(outb.at[src_jp, rs, :], out_ref.at[slot, slot_jp], o_sem.at[0, dst_row], o_sem.at[1, slot], {'row': dst_row})

    def send_out(t):
        ib, jp = block_of(t // hj), t % hj
        for k in range(per_blk):
            dst_row = ib * per_blk + k

            @pl.when(dst_row != me_r)
            def _():
                out_copy(dst_row, jp, me_r, jp).start()

            @pl.when(dst_row == me_r)
            def _():
                out_ref[me_r, jp] = outb[jp, my_rows, :]

    units = cols * hj

    def attend(t):
        ib, jp = block_of(t // hj), t % hj
        t_next = (t + 1) % units
        ib_next, jp_next = block_of(t_next // hj), t_next % hj
        for h in range(heads):
            nxt = (ib, jp, h + 1) if h + 1 < heads else (ib_next, jp_next, 0)
            for _ in zip(scores_steps(*nxt, (h + 1) % 2), softmax_steps(ib, jp, h, h % 2)):
                pass
        outb[jp, pl.ds(pl.multiple_of(ib * tj, tj), tj), :] = jnp.transpose(ga[...]).astype(BF16)

    wait_cols(0)
    project(0)
    f_copy(0, me_c, other).wait_recv()
    for _ in scores_steps(block_of(0), 0, 0, 0):
        pass

    def first_unit(t, _):
        wait_cols(t + 1)
        project(t + 1)

        @pl.when(t > 0)
        def _():
            send_out(t - 1)

        attend(t)
        return 0

    lax.fori_loop(0, hj - 1, first_unit, 0)

    def unit(t, _):
        for phase in range(1, cols):
            @pl.when(t == phase * hj - 1)
            def _():
                blk = block_of(phase)
                d = (me_c - blk + cols) % cols
                f_copy(d, blk, other).wait_recv()

            if phase + 1 < cols:
                @pl.when(t == (phase + 1) * hj - 4)
                def _():
                    blk = block_of(phase + 1)
                    d = (me_c - blk + cols) % cols
                    y_copy(d, blk).wait_recv()
                    f_copy(d, blk, mine).start()

        send_out(t - 1)
        attend(t)
        return 0

    blk = block_of(1)
    y_copy((me_c - blk + cols) % cols, blk).wait_recv()
    f_copy((me_c - blk + cols) % cols, blk, mine).start()
    lax.fori_loop(hj - 1, units, unit, 0)
    send_out(units - 1)

    for d in order:
        x_copy(d, (me_r + d) % rows, me_r).wait_send()
        for jp in range(hj):
            a_copy(d, jp, (me_r + d) % rows, me_r).wait_send()
    for d in y_order:
        y_copy(d, me_c).wait_send()
    for d in range(cols):
        f_copy(d, me_c, mine).wait_send()

    def all_out(send_row, slot):
        rs = pl.ds(pl.multiple_of(send_row * ti, ti), ti)
        return remote(outb.at[:, rs, :], out_ref.at[slot], o_sem.at[0, send_row], o_sem.at[1, slot], {'row': partner})

    for d in order:
        src = (me_r + rows - d) % rows
        all_out(src, src).wait_recv()
    for d in order:
        dst = (me_r + d) % rows
        all_out(dst, dst).wait_send()


def finish_kernel(e, g_ref, z_ref, wo_ref, out_ref, stage):
    rows, hj, ti, lanes = g_ref.shape
    ch, tj = z_ref.shape[1:]
    pitch = ti + PAD
    n_rj = rows * hj
    wo = wo_ref[...].astype(F32)
    z = jnp.zeros((e, ch), F32)
    wo = tr(jnp.concatenate([blk for r in range(0, wo.shape[0], e) for blk in (wo[r:r + e], z)], 0))

    def widen(t, _):
        for jp in range(hj):
            stage[pl.ds(pl.multiple_of((t * hj + jp) * pitch, 8), ti), :] = g_ref[t, jp].astype(F32)
        return 0

    lax.fori_loop(0, rows, widen, 0)

    group = 8

    def step(t, _):
        for q in range(group):
            i = t * group + q
            x = stage[pl.ds(i, n_rj, stride=pitch), :]
            y = pltpu.roll(x, lanes - e, 1)
            x2 = jnp.concatenate([x.reshape(rows, 1, hj, lanes), y.reshape(rows, 1, hj, lanes)], 1).reshape(tj, lanes).astype(BF16)
            out_ref[i] = (mm_nt(wo, x2) + z_ref[i].astype(F32)).astype(BF16)
        return 0

    lax.fori_loop(0, ti // group, step, 0)


VM = pl.BlockSpec(memory_space=pltpu.VMEM)


def solution(mesh):
    rows, cols = mesh.shape['row'], mesh.shape['col']

    def body(pair_tile, res_mask, ln_gamma, ln_beta, w_q, w_k, w_v, w_b, w_g, w_o):
        ti, tj, ch = pair_tile.shape
        heads = w_b.shape[1]
        proj = w_q.shape[1]
        n = ti * rows
        hj = tj // rows // 2
        z = jnp.transpose(pair_tile, (0, 2, 1))
        dma = pltpu.SemaphoreType.DMA
        e = proj // heads
        back = pl.pallas_call(
            functools.partial(triangle_kernel, rows, cols),
            out_shape=jax.ShapeDtypeStruct((rows, hj, ti, 2 * ch), BF16),
            in_specs=[VM] * 9,
            out_specs=VM,
            scratch_shapes=[
                pltpu.VMEM((ti * (rows * hj + PAD), 2 * ch), F32),
                pltpu.VMEM((ti * heads, tj), F32),
                pltpu.VMEM((heads, ti, tj), BF16),
                pltpu.VMEM((rows, hj, ti, 2 * ch), BF16),
                pltpu.VMEM((hj, n, 2 * ch), BF16),
                pltpu.VMEM((cols, heads, n, tj), BF16),
                pltpu.VMEM((hj, cols, heads, 3 * e, 2 * tj), BF16),
                pltpu.VMEM((hj, 2 * proj, n), BF16),
                pltpu.VMEM((hj, cols, 2 * proj, tj), F32),
                pltpu.VMEM((hj, heads, n, 2 * ch), BF16),
                pltpu.VMEM((2, n, 2 * tj), F32),
                pltpu.VMEM((2, 1, 2 * tj), F32),
                pltpu.VMEM((2 * proj, tj), F32),
                pltpu.VMEM((hj, n, 2 * proj), BF16),
                dma((2, hj, rows)), dma((2, rows)), dma((2, cols)), dma((2, cols)), dma((2, rows)),
            ],
            compiler_params=pltpu.CompilerParams(collective_id=0, has_side_effects=True),
            name='triangle',
        )(z, ln_gamma.reshape(1, ch), ln_beta.reshape(1, ch), w_b.T, res_mask.reshape(1, n), w_q, w_k, w_v, w_g)
        out = pl.pallas_call(
            functools.partial(finish_kernel, proj // heads),
            out_shape=jax.ShapeDtypeStruct((ti, ch, tj), BF16),
            in_specs=[VM] * 3,
            out_specs=VM,
            scratch_shapes=[pltpu.VMEM((rows * hj * (ti + PAD), 2 * ch), F32)],
            name='finish',
        )(back, z, w_o)
        return jnp.transpose(out, (0, 2, 1))

    tile_spec = P(('data', 'row'), 'col', None)
    return jax.shard_map(body, mesh=mesh, in_specs=(tile_spec, P('data'), P(), P(), P(), P(), P(), P(), P(), P()), out_specs=tile_spec, check_vma=False)
```

```python
import functools
import math

import jax
import jax.numpy as jnp
import numpy as np
from jax import lax
from jax.experimental import pallas as pl
from jax.experimental.pallas import tpu as pltpu
from jax.sharding import PartitionSpec as P

LN_EPS = 1e-5
MASK_FILL = -1e9
MESH = pl.DeviceIdType.MESH
F32, BF16 = jnp.float32, jnp.bfloat16
NT = (((1,), (1,)), ((), ()))
PAD = 8


def mm(a, b):
    return jnp.dot(a, b, preferred_element_type=F32)


def mm_nt(a, b):
    return lax.dot_general(a, b, NT, preferred_element_type=F32)


def tr(w):
    return jnp.transpose(w.astype(F32)).astype(BF16)


def block_diag2(w):
    z = jnp.zeros_like(w)
    return jnp.concatenate([jnp.concatenate([w, z], 1), jnp.concatenate([z, w], 1)], 0)


def remote(src, dst, send, recv, dev):
    return pltpu.make_async_remote_copy(src_ref=src, dst_ref=dst, send_sem=send, recv_sem=recv, device_id=dev, device_id_type=MESH)


def fill_terms():
    rest, terms = MASK_FILL, []
    for _ in range(3):
        t = float(np.asarray(rest, dtype=BF16))
        terms.append(t)
        rest -= t
    return terms


def pair_rows(wt, e):
    z = jnp.zeros_like(wt)
    lo, hi = jnp.concatenate([wt, z], 1), jnp.concatenate([z, wt], 1)
    return [blk for r in range(0, wt.shape[0], e) for blk in (lo[r:r + e], hi[r:r + e])]


def triangle_kernel(rows, cols, z_ref, gamma_ref, beta_ref, wb_ref, mask_ref, wq_ref, wk_ref, wv_ref, wg_ref, out_ref,
                    stage, bsc, bown, send, a_ref, bias_ref, qp, vt, gt, kh, ss, mm_s, lp, os_, outb, a_sem, x_sem, y_sem, f_sem, o_sem):
    ti, ch, tj = z_ref.shape
    heads = wb_ref.shape[0]
    hj, n, lanes = a_ref.shape
    e = wq_ref.shape[1] // heads
    e2 = 2 * e
    proj2 = 2 * heads * e
    q_scale = 1.0 / math.sqrt(e)
    pitch = rows * hj + PAD
    per_blk = tj // ti
    me_r, me_c = lax.axis_index('row'), lax.axis_index('col')
    core = me_r % 2
    partner = me_r + 1 - 2 * core
    chip = me_r // 2

    barrier = pltpu.get_barrier_semaphore()
    for d in range(1, rows):
        pl.semaphore_signal(barrier, inc=1, device_id={'row': (me_r + d) % rows}, device_id_type=MESH)
    for d in range(1, cols):
        pl.semaphore_signal(barrier, inc=1, device_id={'col': (me_c + d) % cols}, device_id_type=MESH)

    gam = jnp.transpose(jnp.broadcast_to(gamma_ref[...], (tj, ch)))
    bet = jnp.transpose(jnp.broadcast_to(beta_ref[...], (tj, ch)))
    group = 4
    wb = wb_ref[...].astype(F32)
    wb16 = jnp.concatenate([wb] * group, 0)
    wb16 = jnp.concatenate([wb16] * group, 1)
    r_id = lax.broadcasted_iota(jnp.int32, wb16.shape, 0) // heads
    c_id = lax.broadcasted_iota(jnp.int32, wb16.shape, 1) // ch
    wb16 = jnp.where(r_id == c_id, wb16, 0.0).astype(BF16)
    unroll = 2

    def norm_step(t, _):
        for u in range(unroll):
            i0 = (t * unroll + u) * group
            x = z_ref[pl.ds(i0, group)].astype(F32)
            mean = jnp.sum(x, axis=1, keepdims=True) * (1.0 / ch)
            cen = x - mean
            var = jnp.sum(cen * cen, axis=1, keepdims=True) * (1.0 / ch)
            nrm = cen * lax.rsqrt(var + LN_EPS) * gam + bet
            bsc[pl.ds(pl.multiple_of(i0 * heads, group * heads), group * heads), :] = mm(wb16, nrm.astype(BF16).reshape(group * ch, tj))
            for q in range(group):
                t4 = jnp.transpose(nrm[q]).reshape(rows, 2, hj, ch)
                packed = jnp.concatenate([t4[:, 0], t4[:, 1]], axis=-1).reshape(rows * hj, 2 * ch)
                stage[pl.ds(pl.multiple_of((i0 + q) * pitch, 8), rows * hj), :] = packed
        return 0

    lax.fori_loop(0, ti // group // unroll, norm_step, 0)

    my_rows = pl.ds(pl.multiple_of(me_r * ti, ti), ti)
    hh = heads // 2
    mine, other = pl.ds(core * hh, hh), pl.ds((1 - core) * hh, hh)
    for h in range(heads):
        bown[h] = bsc[pl.ds(h, ti, stride=heads), :].astype(BF16)
    bias_ref[me_c, mine, my_rows, :] = bown[mine]

    def x_copy(d, dst_row, src_row):
        rs = pl.ds(pl.multiple_of(src_row * ti, ti), ti)
        part = pl.ds((dst_row % 2) * hh, hh)
        return remote(bown.at[part], bias_ref.at[me_c, part, rs, :], x_sem.at[0, d], x_sem.at[1, d], {'row': (me_r + d) % rows})

    def a_copy(d, jp, dst_row, src_row):
        rs = pl.ds(pl.multiple_of(src_row * ti, ti), ti)
        return remote(send.at[dst_row, jp], a_ref.at[jp, rs, :], a_sem.at[0, jp, d], a_sem.at[1, jp, d], {'row': (me_r + d) % rows})

    def piece(dst_row, jp):
        return stage[pl.ds(dst_row * hj + jp, ti, stride=pitch), :].astype(BF16)

    def y_copy(d, blk):
        return remote(bias_ref.at[blk, mine], bias_ref.at[blk, mine], y_sem.at[0, d], y_sem.at[1, d], {'col': (me_c + d) % cols})

    def f_copy(d, blk, part):
        return remote(bias_ref.at[blk, part], bias_ref.at[blk, part], f_sem.at[0, d], f_sem.at[1, d], {'row': partner})

    order = [4, 3, 5, 2, 6, 1, 7] if rows == 8 else list(range(1, rows))
    y_order = [2, 1, 3] if cols == 4 else list(range(1, cols))

    pl.semaphore_wait(barrier, rows + cols - 2)
    for d in order:
        x_copy(d, (me_r + d) % rows, me_r).start()
    for jp in range(hj + 1):
        if jp < hj:
            for d in order:
                dst = (me_r + d) % rows
                send[dst, jp] = piece(dst, jp)
            a_ref[jp, my_rows, :] = piece(me_r, jp)
        if jp > 0:
            for d in order:
                a_copy(d, jp - 1, (me_r + d) % rows, me_r).start()

    w_qvg = jnp.concatenate(pair_rows(tr(wq_ref[...]), e) + pair_rows(tr(wv_ref[...]), e) + pair_rows(tr(wg_ref[...]), e), 0)
    k_rows = pair_rows(tr(wk_ref[...]), e)
    k_pad = jnp.zeros((lanes - e2, lanes), BF16)
    w_kh = jnp.concatenate([b for h in range(heads) for b in (k_rows[2 * h], k_rows[2 * h + 1], k_pad)], 0)
    masked = jnp.broadcast_to(mask_ref[...] == 0, (lanes, n))
    lane_row = lax.broadcasted_iota(jnp.int32, (lanes, n), 0)
    fill = jnp.zeros((lanes, n), F32)
    for t, f in enumerate(fill_terms()):
        fill = jnp.where(masked & (lane_row == e2 + t), f, fill)
    fill_col = jnp.transpose(fill)
    row_id = lax.broadcasted_iota(jnp.int32, (e, 2 * tj), 0)
    ones_rows = jnp.where(row_id < 3, 1.0, 0.0).astype(BF16)
    eye_r = lax.broadcasted_iota(jnp.int32, (tj, 2 * tj), 0)
    eye_c = lax.broadcasted_iota(jnp.int32, (tj, 2 * tj), 1)
    eye2 = jnp.where(eye_r == lax.rem(eye_c, tj), 1.0, 0.0).astype(BF16)
    z16 = jnp.zeros((e, tj), BF16)
    z_rows = jnp.zeros((lanes - 3 * e, 2 * tj), BF16)

    for d in order:
        x_copy(d, me_r, (me_r + rows - d) % rows).wait_recv()
    f_copy(0, me_c, mine).start()
    for d in y_order:
        y_copy(d, me_c).start()

    def wait_cols(jp):
        for d in order:
            a_copy(d, jp, me_r, (me_r + rows - d) % rows).wait_recv()

    def project(jp):
        a = a_ref[jp]
        r = mm_nt(w_qvg, a)
        q = (r[:proj2] * q_scale).astype(BF16)
        g = jax.nn.sigmoid(r[2 * proj2:])
        vt[jp] = r[proj2:2 * proj2].astype(BF16)
        for ib in range(cols):
            ls = slice(ib * tj, (ib + 1) * tj)
            gt[jp, ib] = g[:, ls]
            for h in range(heads):
                qp[jp, ib, h, 0:e, 0:tj] = q[h * e2:h * e2 + e, ls]
                qp[jp, ib, h, 0:e, tj:2 * tj] = z16
                qp[jp, ib, h, e:e2, 0:tj] = z16
                qp[jp, ib, h, e:e2, tj:2 * tj] = q[h * e2 + e:h * e2 + e2, ls]
                qp[jp, ib, h, e2:3 * e, :] = ones_rows
        k = mm_nt(a, w_kh)
        for h in range(heads):
            kh[jp, h] = (k[:, h * lanes:(h + 1) * lanes] + fill_col).astype(BF16)

    away = [2, 1, 3, 0] if cols == 4 else [(k + 1) % cols for k in range(cols)]
    shift = (me_c - chip + cols) % cols
    pos = sum(jnp.where(shift == a, k, 0) for k, a in enumerate(away))

    def block_of(phase):
        k = jnp.where(phase <= pos, phase - 1, phase)
        step = sum(jnp.where(k == i, a, 0) for i, a in enumerate(away))
        return jnp.where(phase == 0, me_c, (chip + step) % cols)

    halves = 2
    ck = n // halves
    slots = heads

    def scores_dot(ib, jp, h):
        rhs = jnp.concatenate([qp[jp, ib, h], z_rows, eye2], 0)
        return jnp.concatenate([mm(jnp.concatenate([kh[jp, h, c * ck:(c + 1) * ck], bias_ref[ib, h, c * ck:(c + 1) * ck]], 1), rhs) for c in range(halves)], 0)

    def drain(s, c, slot, mx):
        part = s[c * ck:(c + 1) * ck]
        ss[slot, c * ck:(c + 1) * ck] = part
        part = jnp.max(part.reshape(ck // 8, 8, 2 * tj), axis=0)
        return part if mx is None else jnp.maximum(mx, part)

    def weigh(jp, h, slot, c, l, o):
        rs = slice(c * ck, (c + 1) * ck)
        p = jnp.exp(ss[slot, rs] - mm_s[slot])
        part = jnp.sum(p.reshape(ck // 8, 8, 2 * tj), axis=0)
        ob = mm(vt[jp, h * e2:(h + 1) * e2, rs], p.astype(BF16))
        return (part, ob) if l is None else (l + part, o + ob)

    def scores(ib, jp, h):
        s = scores_dot(ib, jp, h)
        mx = None
        for c in range(halves):
            mx = drain(s, c, h, mx)
        mm_s[h] = jnp.max(mx, axis=0, keepdims=True)

    def finish_unit(t):
        ib, jp = block_of(t // hj), t % hj
        parts = []
        for h in range(heads):
            l1 = jnp.sum(lp[h], axis=0, keepdims=True)
            for half in range(2):
                ls = slice(half * tj, (half + 1) * tj)
                rs = slice(h * e2 + half * e, h * e2 + (half + 1) * e)
                parts.append(gt[jp, ib, rs, :] * (os_[h, half * e:(half + 1) * e, ls] / l1[:, ls]))
        outb[jp, pl.ds(pl.multiple_of(ib * tj, tj), tj), :] = jnp.transpose(jnp.concatenate(parts, 0)).astype(BF16)

    def out_copy(dst_row, src_jp, slot, slot_jp):
        rs = pl.ds(pl.multiple_of(dst_row * ti, ti), ti)
        return remote(outb.at[src_jp, rs, :], out_ref.at[slot, slot_jp], o_sem.at[0, dst_row], o_sem.at[1, slot], {'row': dst_row})

    def send_out(t):
        ib, jp = block_of(t // hj), t % hj
        for k in range(per_blk):
            dst_row = ib * per_blk + k

            @pl.when(dst_row != me_r)
            def _():
                out_copy(dst_row, jp, me_r, jp).start()

            @pl.when(dst_row == me_r)
            def _():
                out_ref[me_r, jp] = outb[jp, my_rows, :]

    units = cols * hj

    def attend(t):
        ib, jp = block_of(t // hj), t % hj
        t_next = (t + 1) % units
        ib_next, jp_next = block_of(t_next // hj), t_next % hj
        finish_unit(jnp.maximum(t - 1, 0))
        for h in range(heads):
            nxt = (ib, jp, h + 2) if h + 2 < heads else (ib_next, jp_next, h + 2 - heads)
            s = scores_dot(*nxt)
            l, o, mx = None, None, None
            for c in range(halves):
                mx = drain(s, c, nxt[2], mx)
                l, o = weigh(jp, h, h, c, l, o)

            mm_s[nxt[2]] = jnp.max(mx, axis=0, keepdims=True)
            os_[h] = o
            lp[h] = l

    os_[...] = jnp.ones_like(os_)
    lp[...] = jnp.ones_like(lp)
    wait_cols(0)
    project(0)
    f_copy(0, me_c, other).wait_recv()
    for h in range(2):
        scores(me_c, 0, h)

    def first_unit(t, _):
        wait_cols(t + 1)
        project(t + 1)

        @pl.when(t > 1)
        def _():
            send_out(t - 2)

        attend(t)
        return 0

    lax.fori_loop(0, hj - 1, first_unit, 0)

    def unit(t, _):
        for phase in range(1, cols):
            @pl.when(t == phase * hj - 1)
            def _():
                blk = block_of(phase)
                d = (me_c - blk + cols) % cols
                f_copy(d, blk, other).wait_recv()

            if phase + 1 < cols:
                @pl.when(t == (phase + 1) * hj - 4)
                def _():
                    blk = block_of(phase + 1)
                    d = (me_c - blk + cols) % cols
                    y_copy(d, blk).wait_recv()
                    f_copy(d, blk, mine).start()

        send_out(t - 2)
        attend(t)
        return 0

    blk = block_of(1)
    y_copy((me_c - blk + cols) % cols, blk).wait_recv()
    f_copy((me_c - blk + cols) % cols, blk, mine).start()
    lax.fori_loop(hj - 1, units, unit, 0)
    finish_unit(units - 1)
    send_out(units - 2)
    send_out(units - 1)

    for d in order:
        x_copy(d, (me_r + d) % rows, me_r).wait_send()
        for jp in range(hj):
            a_copy(d, jp, (me_r + d) % rows, me_r).wait_send()
    for d in y_order:
        y_copy(d, me_c).wait_send()
    for d in range(cols):
        f_copy(d, me_c, mine).wait_send()

    def all_out(send_row, slot):
        rs = pl.ds(pl.multiple_of(send_row * ti, ti), ti)
        return remote(outb.at[:, rs, :], out_ref.at[slot], o_sem.at[0, send_row], o_sem.at[1, slot], {'row': partner})

    for d in order:
        src = (me_r + rows - d) % rows
        all_out(src, src).wait_recv()
    for d in order:
        dst = (me_r + d) % rows
        all_out(dst, dst).wait_send()


def finish_kernel(e, g_ref, z_ref, wo_ref, out_ref, stage):
    rows, hj, ti, lanes = g_ref.shape
    ch, tj = z_ref.shape[1:]
    pitch = ti + PAD
    n_rj = rows * hj
    wo = wo_ref[...].astype(F32)
    z = jnp.zeros((e, ch), F32)
    wo = tr(jnp.concatenate([blk for r in range(0, wo.shape[0], e) for blk in (wo[r:r + e], z)], 0))

    def widen(t, _):
        for jp in range(hj):
            stage[pl.ds(pl.multiple_of((t * hj + jp) * pitch, 8), ti), :] = g_ref[t, jp].astype(F32)
        return 0

    lax.fori_loop(0, rows, widen, 0)

    group = 8

    def step(t, _):
        for q in range(group):
            i = t * group + q
            x = stage[pl.ds(i, n_rj, stride=pitch), :]
            y = pltpu.roll(x, lanes - e, 1)
            x2 = jnp.concatenate([x.reshape(rows, 1, hj, lanes), y.reshape(rows, 1, hj, lanes)], 1).reshape(tj, lanes).astype(BF16)
            out_ref[i] = (mm_nt(wo, x2) + z_ref[i].astype(F32)).astype(BF16)
        return 0

    lax.fori_loop(0, ti // group, step, 0)


VM = pl.BlockSpec(memory_space=pltpu.VMEM)


def solution(mesh):
    rows, cols = mesh.shape['row'], mesh.shape['col']

    def body(pair_tile, res_mask, ln_gamma, ln_beta, w_q, w_k, w_v, w_b, w_g, w_o):
        ti, tj, ch = pair_tile.shape
        heads = w_b.shape[1]
        proj = w_q.shape[1]
        n = ti * rows
        hj = tj // rows // 2
        z = jnp.transpose(pair_tile, (0, 2, 1))
        dma = pltpu.SemaphoreType.DMA
        e = proj // heads
        back = pl.pallas_call(
            functools.partial(triangle_kernel, rows, cols),
            out_shape=jax.ShapeDtypeStruct((rows, hj, ti, 2 * ch), BF16),
            in_specs=[VM] * 9,
            out_specs=VM,
            scratch_shapes=[
                pltpu.VMEM((ti * (rows * hj + PAD), 2 * ch), F32),
                pltpu.VMEM((ti * heads, tj), F32),
                pltpu.VMEM((heads, ti, tj), BF16),
                pltpu.VMEM((rows, hj, ti, 2 * ch), BF16),
                pltpu.VMEM((hj, n, 2 * ch), BF16),
                pltpu.VMEM((cols, heads, n, tj), BF16),
                pltpu.VMEM((hj, cols, heads, 3 * e, 2 * tj), BF16),
                pltpu.VMEM((hj, 2 * proj, n), BF16),
                pltpu.VMEM((hj, cols, 2 * proj, tj), F32),
                pltpu.VMEM((hj, heads, n, 2 * ch), BF16),
                pltpu.VMEM((heads, n, 2 * tj), F32),
                pltpu.VMEM((heads, 1, 2 * tj), F32),
                pltpu.VMEM((heads, 8, 2 * tj), F32),
                pltpu.VMEM((heads, 2 * e, 2 * tj), F32),
                pltpu.VMEM((hj, n, 2 * proj), BF16),
                dma((2, hj, rows)), dma((2, rows)), dma((2, cols)), dma((2, cols)), dma((2, rows)),
            ],
            compiler_params=pltpu.CompilerParams(collective_id=0, has_side_effects=True),
            name='triangle',
        )(z, ln_gamma.reshape(1, ch), ln_beta.reshape(1, ch), w_b.T, res_mask.reshape(1, n), w_q, w_k, w_v, w_g)
        out = pl.pallas_call(
            functools.partial(finish_kernel, proj // heads),
            out_shape=jax.ShapeDtypeStruct((ti, ch, tj), BF16),
            in_specs=[VM] * 3,
            out_specs=VM,
            scratch_shapes=[pltpu.VMEM((rows * hj * (ti + PAD), 2 * ch), F32)],
            name='finish',
        )(back, z, w_o)
        return jnp.transpose(out, (0, 2, 1))

    tile_spec = P(('data', 'row'), 'col', None)
    return jax.shard_map(body, mesh=mesh, in_specs=(tile_spec, P('data'), P(), P(), P(), P(), P(), P(), P(), P()), out_specs=tile_spec, check_vma=False)
```

```python
import functools
import math

import jax
import jax.numpy as jnp
import numpy as np
from jax import lax
from jax.experimental import pallas as pl
from jax.experimental.pallas import tpu as pltpu
from jax.sharding import PartitionSpec as P

LN_EPS = 1e-5
MASK_FILL = -1e9
MESH = pl.DeviceIdType.MESH
F32, BF16 = jnp.float32, jnp.bfloat16
NT = (((1,), (1,)), ((), ()))
PAD = 8


def mm(a, b):
    return jnp.dot(a, b, preferred_element_type=F32)


def mm_nt(a, b):
    return lax.dot_general(a, b, NT, preferred_element_type=F32)


def tr(w):
    return jnp.transpose(w.astype(F32)).astype(BF16)


def block_diag2(w):
    z = jnp.zeros_like(w)
    return jnp.concatenate([jnp.concatenate([w, z], 1), jnp.concatenate([z, w], 1)], 0)


def remote(src, dst, send, recv, dev):
    return pltpu.make_async_remote_copy(src_ref=src, dst_ref=dst, send_sem=send, recv_sem=recv, device_id=dev, device_id_type=MESH)


def fill_terms():
    rest, terms = MASK_FILL, []
    for _ in range(3):
        t = float(np.asarray(rest, dtype=BF16))
        terms.append(t)
        rest -= t
    return terms


def pair_rows(wt, e):
    z = jnp.zeros_like(wt)
    lo, hi = jnp.concatenate([wt, z], 1), jnp.concatenate([z, wt], 1)
    return [blk for r in range(0, wt.shape[0], e) for blk in (lo[r:r + e], hi[r:r + e])]


def triangle_kernel(rows, cols, z_ref, gamma_ref, beta_ref, wb_ref, mask_ref, wq_ref, wk_ref, wv_ref, wg_ref, out_ref,
                    stage, bsc, bown, send, a_ref, bias_ref, qp, vt, gt, kh, ss, mm_s, lp, os_, outb, a_sem, x_sem, y_sem, f_sem, g_sem, o_sem):
    ti, ch, tj = z_ref.shape
    heads = wb_ref.shape[0]
    hj, n, lanes = a_ref.shape
    e = wq_ref.shape[1] // heads
    e2 = 2 * e
    proj2 = 2 * heads * e
    q_scale = 1.0 / math.sqrt(e)
    pitch = rows * hj + PAD
    per_blk = tj // ti
    me_r, me_c = lax.axis_index('row'), lax.axis_index('col')
    core = me_r % 2
    partner = me_r + 1 - 2 * core
    chip = me_r // 2

    barrier = pltpu.get_barrier_semaphore()
    for d in range(1, rows):
        pl.semaphore_signal(barrier, inc=1, device_id={'row': (me_r + d) % rows}, device_id_type=MESH)
    for d in range(1, cols):
        pl.semaphore_signal(barrier, inc=1, device_id={'col': (me_c + d) % cols}, device_id_type=MESH)

    gam = jnp.transpose(jnp.broadcast_to(gamma_ref[...], (tj, ch)))
    bet = jnp.transpose(jnp.broadcast_to(beta_ref[...], (tj, ch)))
    group = 4
    wb = wb_ref[...].astype(F32)
    wb16 = jnp.concatenate([wb] * group, 0)
    wb16 = jnp.concatenate([wb16] * group, 1)
    r_id = lax.broadcasted_iota(jnp.int32, wb16.shape, 0) // heads
    c_id = lax.broadcasted_iota(jnp.int32, wb16.shape, 1) // ch
    wb16 = jnp.where(r_id == c_id, wb16, 0.0).astype(BF16)
    unroll = 4

    def norm_step(t, _):
        for u in range(unroll):
            i0 = (t * unroll + u) * group
            x = z_ref[pl.ds(i0, group)].astype(F32)
            mean = jnp.sum(x, axis=1, keepdims=True) * (1.0 / ch)
            cen = x - mean
            var = jnp.sum(cen * cen, axis=1, keepdims=True) * (1.0 / ch)
            nrm = cen * lax.rsqrt(var + LN_EPS) * gam + bet
            bsc[pl.ds(pl.multiple_of(i0 * heads, group * heads), group * heads), :] = mm(wb16, nrm.astype(BF16).reshape(group * ch, tj))
            for q in range(group):
                t4 = jnp.transpose(nrm[q]).reshape(rows, 2, hj, ch)
                packed = jnp.concatenate([t4[:, 0], t4[:, 1]], axis=-1).reshape(rows * hj, 2 * ch)
                stage[pl.ds(pl.multiple_of((i0 + q) * pitch, 8), rows * hj), :] = packed
        return 0

    lax.fori_loop(0, ti // group // unroll, norm_step, 0)

    my_rows = pl.ds(pl.multiple_of(me_r * ti, ti), ti)
    hh = heads // 2
    mine, other = pl.ds(core * hh, hh), pl.ds((1 - core) * hh, hh)
    for h in range(heads):
        bown[h] = bsc[pl.ds(h, ti, stride=heads), :].astype(BF16)
    bias_ref[me_c, mine, my_rows, :] = bown[mine]

    def x_copy(d, dst_row, src_row):
        rs = pl.ds(pl.multiple_of(src_row * ti, ti), ti)
        part = pl.ds((dst_row % 2) * hh, hh)
        return remote(bown.at[part], bias_ref.at[me_c, part, rs, :], x_sem.at[0, d], x_sem.at[1, d], {'row': (me_r + d) % rows})

    def a_copy(d, jp, dst_row, src_row):
        rs = pl.ds(pl.multiple_of(src_row * ti, ti), ti)
        return remote(send.at[dst_row, jp], a_ref.at[jp, rs, :], a_sem.at[0, jp, d], a_sem.at[1, jp, d], {'row': (me_r + d) % rows})

    def piece(dst_row, jp):
        return stage[pl.ds(dst_row * hj + jp, ti, stride=pitch), :].astype(BF16)

    def y_copy(d, blk):
        return remote(bias_ref.at[blk, mine], bias_ref.at[blk, mine], y_sem.at[0, d], y_sem.at[1, d], {'col': (me_c + d) % cols})

    def f_copy(d, blk, part):
        return remote(bias_ref.at[blk, part], bias_ref.at[blk, part], f_sem.at[0, d], f_sem.at[1, d], {'row': partner})

    order = [4, 3, 5, 2, 6, 1, 7] if rows == 8 else list(range(1, rows))
    y_order = [1, cols - 1]

    pl.semaphore_wait(barrier, rows + cols - 2)
    for d in order:
        x_copy(d, (me_r + d) % rows, me_r).start()
    for jp in range(hj + 1):
        if jp < hj:
            for d in order:
                dst = (me_r + d) % rows
                send[dst, jp] = piece(dst, jp)
            a_ref[jp, my_rows, :] = piece(me_r, jp)
        if jp > 0:
            for d in order:
                a_copy(d, jp - 1, (me_r + d) % rows, me_r).start()

    w_qvg = jnp.concatenate(pair_rows(tr(wq_ref[...]), e) + pair_rows(tr(wv_ref[...]), e) + pair_rows(tr(wg_ref[...]), e), 0)
    k_rows = pair_rows(tr(wk_ref[...]), e)
    k_pad = jnp.zeros((lanes - e2, lanes), BF16)
    w_kh = jnp.concatenate([b for h in range(heads) for b in (k_rows[2 * h], k_rows[2 * h + 1], k_pad)], 0)
    masked = jnp.broadcast_to(mask_ref[...] == 0, (lanes, n))
    lane_row = lax.broadcasted_iota(jnp.int32, (lanes, n), 0)
    fill = jnp.zeros((lanes, n), F32)
    for t, f in enumerate(fill_terms()):
        fill = jnp.where(masked & (lane_row == e2 + t), f, fill)
    fill_col = jnp.transpose(fill)
    row_id = lax.broadcasted_iota(jnp.int32, (e, 2 * tj), 0)
    ones_rows = jnp.where(row_id < 3, 1.0, 0.0).astype(BF16)
    eye_r = lax.broadcasted_iota(jnp.int32, (tj, 2 * tj), 0)
    eye_c = lax.broadcasted_iota(jnp.int32, (tj, 2 * tj), 1)
    eye2 = jnp.where(eye_r == lax.rem(eye_c, tj), 1.0, 0.0).astype(BF16)
    z16 = jnp.zeros((e, tj), BF16)
    z_rows = jnp.zeros((lanes - 3 * e, 2 * tj), BF16)

    for d in order:
        x_copy(d, me_r, (me_r + rows - d) % rows).wait_recv()
    f_copy(0, me_c, mine).start()
    for d in y_order:
        y_copy(d, me_c).start()

    def wait_cols(jp):
        for d in order:
            a_copy(d, jp, me_r, (me_r + rows - d) % rows).wait_recv()

    def project(jp):
        a = a_ref[jp]
        r = mm_nt(w_qvg, a)
        q = (r[:proj2] * q_scale).astype(BF16)
        g = jax.nn.sigmoid(r[2 * proj2:])
        vt[jp] = r[proj2:2 * proj2].astype(BF16)
        for ib in range(cols):
            ls = slice(ib * tj, (ib + 1) * tj)
            gt[jp, ib] = g[:, ls]
            for h in range(heads):
                qp[jp, ib, h, 0:e, 0:tj] = q[h * e2:h * e2 + e, ls]
                qp[jp, ib, h, 0:e, tj:2 * tj] = z16
                qp[jp, ib, h, e:e2, 0:tj] = z16
                qp[jp, ib, h, e:e2, tj:2 * tj] = q[h * e2 + e:h * e2 + e2, ls]
                qp[jp, ib, h, e2:3 * e, :] = ones_rows
        k = mm_nt(a, w_kh)
        for h in range(heads):
            kh[jp, h] = (k[:, h * lanes:(h + 1) * lanes] + fill_col).astype(BF16)

    blk_a, blk_b, blk_d = (me_c + 1) % cols, (me_c + cols - 1) % cols, (me_c + 2) % cols

    halves = 2
    ck = n // halves
    slots = heads

    def scores_dot(ib, jp, h):
        rhs = jnp.concatenate([qp[jp, ib, h], z_rows, eye2], 0)
        return jnp.concatenate([mm(jnp.concatenate([kh[jp, h, c * ck:(c + 1) * ck], bias_ref[ib, h, c * ck:(c + 1) * ck]], 1), rhs) for c in range(halves)], 0)

    def drain(s, c, slot, mx):
        part = s[c * ck:(c + 1) * ck]
        ss[slot, c * ck:(c + 1) * ck] = part
        part = jnp.max(part.reshape(ck // 8, 8, 2 * tj), axis=0)
        return part if mx is None else jnp.maximum(mx, part)

    def weigh(jp, h, slot, c, l, o):
        rs = slice(c * ck, (c + 1) * ck)
        p = jnp.exp(ss[slot, rs] - mm_s[slot])
        part = jnp.sum(p.reshape(ck // 8, 8, 2 * tj), axis=0)
        ob = mm(vt[jp, h * e2:(h + 1) * e2, rs], p.astype(BF16))
        return (part, ob) if l is None else (l + part, o + ob)

    def scores(ib, jp, h):
        s = scores_dot(ib, jp, h)
        mx = None
        for c in range(halves):
            mx = drain(s, c, h, mx)
        mm_s[h] = jnp.max(mx, axis=0, keepdims=True)

    def finish_unit(jp, ib):
        parts = []
        for h in range(heads):
            l1 = jnp.sum(lp[h], axis=0, keepdims=True)
            for half in range(2):
                ls = slice(half * tj, (half + 1) * tj)
                rs = slice(h * e2 + half * e, h * e2 + (half + 1) * e)
                parts.append(gt[jp, ib, rs, :] * (os_[h, half * e:(half + 1) * e, ls] / l1[:, ls]))
        outb[jp, pl.ds(pl.multiple_of(ib * tj, tj), tj), :] = jnp.transpose(jnp.concatenate(parts, 0)).astype(BF16)

    def out_copy(dst_row, src_jp, slot, slot_jp):
        rs = pl.ds(pl.multiple_of(dst_row * ti, ti), ti)
        return remote(outb.at[src_jp, rs, :], out_ref.at[slot, slot_jp], o_sem.at[0, dst_row], o_sem.at[1, slot], {'row': dst_row})

    def send_out(jp, ib):
        for k in range(per_blk):
            dst_row = ib * per_blk + k

            @pl.when(dst_row != me_r)
            def _():
                out_copy(dst_row, jp, me_r, jp).start()

            @pl.when(dst_row == me_r)
            def _():
                out_ref[me_r, jp] = outb[jp, my_rows, :]

    def attend(jp, ib, jp_prev, ib_prev, jp_next, ib_next):
        finish_unit(jp_prev, ib_prev)
        for h in range(heads):
            nxt = (ib, jp, h + 2) if h + 2 < heads else (ib_next, jp_next, h + 2 - heads)
            s = scores_dot(*nxt)
            l, o, mx = None, None, None
            for c in range(halves):
                mx = drain(s, c, nxt[2], mx)
                l, o = weigh(jp, h, h, c, l, o)
            mm_s[nxt[2]] = jnp.max(mx, axis=0, keepdims=True)
            os_[h] = o
            lp[h] = l

    os_[...] = jnp.ones_like(os_)
    lp[...] = jnp.ones_like(lp)
    wait_cols(0)
    project(0)
    f_copy(0, me_c, other).wait_recv()
    for h in range(2):
        scores(me_c, 0, h)

    def bring(blk):
        d = (me_c - blk + cols) % cols
        y_copy(d, blk).wait_recv()
        f_copy(d, blk, mine).start()

    def relay(side, blk, step):
        part = pl.ds(core * hh + side * (hh // 2), hh // 2)
        return remote(bias_ref.at[blk, part], bias_ref.at[blk, part], g_sem.at[0, side], g_sem.at[1, side], {'col': (me_c + step) % cols})

    def brought(blk):
        f_copy((me_c - blk + cols) % cols, blk, other).wait_recv()

    def chain(units, prev, nxt):
        seq = [prev] + units + [nxt]
        for k in range(1, len(seq) - 1):
            attend(*seq[k], *seq[k - 1], *seq[k + 1])

    def pick(cond, yes, no):
        return tuple(jnp.where(cond, y, n) for y, n in zip(yes, no))

    n_a = hj // 2

    def lead_in(t, _):
        wait_cols(t + 1)
        project(t + 1)

        @pl.when(t == n_a - 1)
        def _():
            bring(blk_a)
            relay(0, blk_a, cols - 1).start()
            bring(blk_b)
            relay(1, blk_b, 1).start()

        chain([(t, me_c)], (jnp.maximum(t - 1, 0), me_c), (t + 1, me_c))
        return 0

    lax.fori_loop(0, n_a, lead_in, 0)
    brought(blk_a)
    brought(blk_b)

    def send_earlier(t):
        @pl.when(t == n_a)
        def _():
            for k in range(n_a - 1):
                send_out(k, me_c)

        @pl.when(t > n_a)
        def _():
            send_out(*pick(t == n_a + 1, (n_a - 1, me_c), (t - n_a - 2, blk_b)))
            send_out(t - 1, me_c)
            send_out(t - n_a - 1, blk_a)

    def three(t, _):
        wait_cols(t + 1)
        project(t + 1)
        send_earlier(t)
        chain([(t, me_c), (t - n_a, blk_a), (t - n_a, blk_b)], pick(t == n_a, (t - 1, me_c), (t - n_a - 1, blk_b)), (t + 1, me_c))
        return 0

    lax.fori_loop(n_a, hj - 1, three, 0)
    relay(0, blk_d, cols - 1).wait_recv()
    relay(1, blk_d, 1).wait_recv()
    f_copy(2, blk_d, mine).start()

    def bridge(t, _):
        send_earlier(t)
        chain([(t, me_c), (t - n_a, blk_a), (t - n_a, blk_b)], (t - n_a - 1, blk_b), (n_a, blk_a))
        return 0

    lax.fori_loop(hj - 1, hj, bridge, 0)
    brought(blk_d)

    def four(s, _):
        @pl.when(s == 0)
        def _():
            send_out(n_a - 2, blk_b)
            send_out(hj - 1, me_c)
            send_out(n_a - 1, blk_a)

        @pl.when(s > 0)
        def _():
            send_out(*pick(s == 1, (n_a - 1, blk_b), (2 * s - 3, blk_d)))
            send_out(n_a - 1 + s, blk_a)
            send_out(2 * s - 2, blk_d)
            send_out(n_a - 1 + s, blk_b)

        chain([(n_a + s, blk_a), (2 * s, blk_d), (n_a + s, blk_b), (2 * s + 1, blk_d)],
              pick(s == 0, (n_a - 1, blk_b), (2 * s - 1, blk_d)), (jnp.minimum(n_a + 1 + s, hj - 1), blk_a))
        return 0

    lax.fori_loop(0, hj - n_a, four, 0)
    send_out(hj - 3, blk_d)
    send_out(hj - 1, blk_a)
    send_out(hj - 2, blk_d)
    send_out(hj - 1, blk_b)
    finish_unit(hj - 1, blk_d)
    send_out(hj - 1, blk_d)

    for d in order:
        x_copy(d, (me_r + d) % rows, me_r).wait_send()
        for jp in range(hj):
            a_copy(d, jp, (me_r + d) % rows, me_r).wait_send()
    for d in y_order:
        y_copy(d, me_c).wait_send()
    relay(0, blk_a, cols - 1).wait_send()
    relay(1, blk_b, 1).wait_send()
    for d in range(cols):
        f_copy(d, me_c, mine).wait_send()

    def all_out(send_row, slot):
        rs = pl.ds(pl.multiple_of(send_row * ti, ti), ti)
        return remote(outb.at[:, rs, :], out_ref.at[slot], o_sem.at[0, send_row], o_sem.at[1, slot], {'row': partner})

    for d in order:
        src = (me_r + rows - d) % rows
        all_out(src, src).wait_recv()
    for d in order:
        dst = (me_r + d) % rows
        all_out(dst, dst).wait_send()


def finish_kernel(e, g_ref, z_ref, wo_ref, out_ref, stage):
    rows, hj, ti, lanes = g_ref.shape
    ch, tj = z_ref.shape[1:]
    pitch = ti + PAD
    n_rj = rows * hj
    wo = wo_ref[...].astype(F32)
    z = jnp.zeros((e, ch), F32)
    wo = tr(jnp.concatenate([blk for r in range(0, wo.shape[0], e) for blk in (wo[r:r + e], z)], 0))
    for rj in range(n_rj):
        stage[rj * pitch:rj * pitch + ti, :] = g_ref[rj // hj, rj % hj].astype(F32)
    for i in range(ti):
        x = stage[pl.ds(i, n_rj, stride=pitch), :]
        y = pltpu.roll(x, lanes - e, 1)
        x2 = jnp.concatenate([x.reshape(rows, 1, hj, lanes), y.reshape(rows, 1, hj, lanes)], 1).reshape(tj, lanes).astype(BF16)
        out_ref[i] = (mm_nt(wo, x2) + z_ref[i].astype(F32)).astype(BF16)


VM = pl.BlockSpec(memory_space=pltpu.VMEM)


def solution(mesh):
    rows, cols = mesh.shape['row'], mesh.shape['col']

    def body(pair_tile, res_mask, ln_gamma, ln_beta, w_q, w_k, w_v, w_b, w_g, w_o):
        ti, tj, ch = pair_tile.shape
        heads = w_b.shape[1]
        proj = w_q.shape[1]
        n = ti * rows
        hj = tj // rows // 2
        z = jnp.transpose(pair_tile, (0, 2, 1))
        dma = pltpu.SemaphoreType.DMA
        e = proj // heads
        back = pl.pallas_call(
            functools.partial(triangle_kernel, rows, cols),
            out_shape=jax.ShapeDtypeStruct((rows, hj, ti, 2 * ch), BF16),
            in_specs=[VM] * 9,
            out_specs=VM,
            scratch_shapes=[
                pltpu.VMEM((ti * (rows * hj + PAD), 2 * ch), F32),
                pltpu.VMEM((ti * heads, tj), F32),
                pltpu.VMEM((heads, ti, tj), BF16),
                pltpu.VMEM((rows, hj, ti, 2 * ch), BF16),
                pltpu.VMEM((hj, n, 2 * ch), BF16),
                pltpu.VMEM((cols, heads, n, tj), BF16),
                pltpu.VMEM((hj, cols, heads, 3 * e, 2 * tj), BF16),
                pltpu.VMEM((hj, 2 * proj, n), BF16),
                pltpu.VMEM((hj, cols, 2 * proj, tj), F32),
                pltpu.VMEM((hj, heads, n, 2 * ch), BF16),
                pltpu.VMEM((heads, n, 2 * tj), F32),
                pltpu.VMEM((heads, 1, 2 * tj), F32),
                pltpu.VMEM((heads, 8, 2 * tj), F32),
                pltpu.VMEM((heads, 2 * e, 2 * tj), F32),
                pltpu.VMEM((hj, n, 2 * proj), BF16),
                dma((2, hj, rows)), dma((2, rows)), dma((2, cols)), dma((2, cols)), dma((2, 2)), dma((2, rows)),
            ],
            compiler_params=pltpu.CompilerParams(collective_id=0, has_side_effects=True),
            name='triangle',
        )(z, ln_gamma.reshape(1, ch), ln_beta.reshape(1, ch), w_b.T, res_mask.reshape(1, n), w_q, w_k, w_v, w_g)
        chunk = ti // 4
        out = pl.pallas_call(
            functools.partial(finish_kernel, proj // heads),
            out_shape=jax.ShapeDtypeStruct((ti, ch, tj), BF16),
            grid=(ti // chunk,),
            in_specs=[
                pl.BlockSpec((rows, hj, chunk, 2 * ch), lambda i: (0, 0, i, 0)),
                pl.BlockSpec((chunk, ch, tj), lambda i: (i, 0, 0)),
                pl.BlockSpec((proj, ch), lambda i: (0, 0)),
            ],
            out_specs=pl.BlockSpec((chunk, ch, tj), lambda i: (i, 0, 0)),
            scratch_shapes=[pltpu.VMEM((rows * hj * (chunk + PAD), 2 * ch), F32)],
            name='finish',
        )(back, z, w_o)
        return jnp.transpose(out, (0, 2, 1))

    tile_spec = P(('data', 'row'), 'col', None)
    return jax.shard_map(body, mesh=mesh, in_specs=(tile_spec, P('data'), P(), P(), P(), P(), P(), P(), P(), P()), out_specs=tile_spec, check_vma=False)
```

```python
import functools
import math

import jax
import jax.numpy as jnp
import numpy as np
from jax import lax
from jax.experimental import pallas as pl
from jax.experimental.pallas import tpu as pltpu
from jax.sharding import PartitionSpec as P

LN_EPS = 1e-5
MASK_FILL = -1e9
MESH = pl.DeviceIdType.MESH
F32, BF16 = jnp.float32, jnp.bfloat16
NT = (((1,), (1,)), ((), ()))
PAD = 8


def mm(a, b):
    return jnp.dot(a, b, preferred_element_type=F32)


def mm_nt(a, b):
    return lax.dot_general(a, b, NT, preferred_element_type=F32)


def tr(w):
    return jnp.transpose(w.astype(F32)).astype(BF16)


def block_diag2(w):
    z = jnp.zeros_like(w)
    return jnp.concatenate([jnp.concatenate([w, z], 1), jnp.concatenate([z, w], 1)], 0)


def remote(src, dst, send, recv, dev):
    return pltpu.make_async_remote_copy(src_ref=src, dst_ref=dst, send_sem=send, recv_sem=recv, device_id=dev, device_id_type=MESH)


def fill_terms():
    rest, terms = MASK_FILL, []
    for _ in range(3):
        t = float(np.asarray(rest, dtype=BF16))
        terms.append(t)
        rest -= t
    return terms


def pair_rows(wt, e):
    z = jnp.zeros_like(wt)
    lo, hi = jnp.concatenate([wt, z], 1), jnp.concatenate([z, wt], 1)
    return [blk for r in range(0, wt.shape[0], e) for blk in (lo[r:r + e], hi[r:r + e])]


def triangle_kernel(rows, cols, z_ref, gamma_ref, beta_ref, wb_ref, mask_ref, wq_ref, wk_ref, wv_ref, wg_ref, out_ref,
                    stage, bsc, bown, send, a_ref, bias_ref, qp, vt, gt, kh, ss, mm_s, lp, os_, outb, a_sem, x_sem, y_sem, f_sem, g_sem, o_sem, l_sem):
    ti, ch, tj = z_ref.shape
    heads = wb_ref.shape[0]
    hj, n, lanes = a_ref.shape
    e = wq_ref.shape[1] // heads
    e2 = 2 * e
    proj2 = 2 * heads * e
    q_scale = 1.0 / math.sqrt(e)
    pitch = rows * hj + PAD
    per_blk = tj // ti
    me_r, me_c = lax.axis_index('row'), lax.axis_index('col')
    core = me_r % 2
    partner = me_r + 1 - 2 * core
    chip = me_r // 2

    barrier = pltpu.get_barrier_semaphore()
    for d in range(1, rows):
        pl.semaphore_signal(barrier, inc=1, device_id={'row': (me_r + d) % rows}, device_id_type=MESH)
    for d in range(1, cols):
        pl.semaphore_signal(barrier, inc=1, device_id={'col': (me_c + d) % cols}, device_id_type=MESH)

    gam = jnp.transpose(jnp.broadcast_to(gamma_ref[...], (tj, ch)))
    bet = jnp.transpose(jnp.broadcast_to(beta_ref[...], (tj, ch)))
    group = 4
    wb = wb_ref[...].astype(F32)
    wb16 = jnp.concatenate([wb] * group, 0)
    wb16 = jnp.concatenate([wb16] * group, 1)
    r_id = lax.broadcasted_iota(jnp.int32, wb16.shape, 0) // heads
    c_id = lax.broadcasted_iota(jnp.int32, wb16.shape, 1) // ch
    wb16 = jnp.where(r_id == c_id, wb16, 0.0).astype(BF16)
    unroll = 4

    def norm_step(t, _):
        for u in range(unroll):
            i0 = (t * unroll + u) * group
            x = z_ref[pl.ds(i0, group)].astype(F32)
            mean = jnp.sum(x, axis=1, keepdims=True) * (1.0 / ch)
            cen = x - mean
            var = jnp.sum(cen * cen, axis=1, keepdims=True) * (1.0 / ch)
            nrm = cen * lax.rsqrt(var + LN_EPS) * gam + bet
            bsc[pl.ds(pl.multiple_of(i0 * heads, group * heads), group * heads), :] = mm(wb16, nrm.astype(BF16).reshape(group * ch, tj))
            for q in range(group):
                t4 = jnp.transpose(nrm[q]).reshape(rows, 2, hj, ch)
                packed = jnp.concatenate([t4[:, 0], t4[:, 1]], axis=-1).reshape(rows * hj, 2 * ch)
                stage[pl.ds(pl.multiple_of((i0 + q) * pitch, 8), rows * hj), :] = packed
        return 0

    lax.fori_loop(0, ti // group // unroll, norm_step, 0)

    my_rows = pl.ds(pl.multiple_of(me_r * ti, ti), ti)
    hh = heads // 2
    mine, other = pl.ds(core * hh, hh), pl.ds((1 - core) * hh, hh)
    for h in range(heads):
        bown[h] = bsc[pl.ds(h, ti, stride=heads), :].astype(BF16)
    bias_ref[me_c, mine, my_rows, :] = bown[mine]

    def x_copy(d, dst_row, src_row):
        rs = pl.ds(pl.multiple_of(src_row * ti, ti), ti)
        part = pl.ds((dst_row % 2) * hh, hh)
        return remote(bown.at[part], bias_ref.at[me_c, part, rs, :], x_sem.at[0, d], x_sem.at[1, d], {'row': (me_r + d) % rows})

    def a_copy(d, jp, dst_row, src_row):
        rs = pl.ds(pl.multiple_of(src_row * ti, ti), ti)
        return remote(send.at[dst_row, jp], a_ref.at[jp, rs, :], a_sem.at[0, jp, d], a_sem.at[1, jp, d], {'row': (me_r + d) % rows})

    def piece(dst_row, jp):
        return stage[pl.ds(dst_row * hj + jp, ti, stride=pitch), :].astype(BF16)

    def y_copy(d, blk):
        return remote(bias_ref.at[blk, mine], bias_ref.at[blk, mine], y_sem.at[0, d], y_sem.at[1, d], {'col': (me_c + d) % cols})

    def f_copy(d, blk, part):
        return remote(bias_ref.at[blk, part], bias_ref.at[blk, part], f_sem.at[0, d], f_sem.at[1, d], {'row': partner})

    order = [4, 3, 5, 2, 6, 1, 7] if rows == 8 else list(range(1, rows))
    y_order = [1, cols - 1]

    pl.semaphore_wait(barrier, rows + cols - 2)
    for d in order:
        x_copy(d, (me_r + d) % rows, me_r).start()
    for jp in range(hj + 1):
        if jp < hj:
            for d in order:
                dst = (me_r + d) % rows
                send[dst, jp] = piece(dst, jp)
            a_ref[jp, my_rows, :] = piece(me_r, jp)
        if jp > 0:
            for d in order:
                a_copy(d, jp - 1, (me_r + d) % rows, me_r).start()

    w_qvg = jnp.concatenate(pair_rows(tr(wq_ref[...]), e) + pair_rows(tr(wv_ref[...]), e) + pair_rows(tr(wg_ref[...]), e), 0)
    k_rows = pair_rows(tr(wk_ref[...]), e)
    k_pad = jnp.zeros((lanes - e2, lanes), BF16)
    w_kh = jnp.concatenate([b for h in range(heads) for b in (k_rows[2 * h], k_rows[2 * h + 1], k_pad)], 0)
    masked = jnp.broadcast_to(mask_ref[...] == 0, (lanes, n))
    lane_row = lax.broadcasted_iota(jnp.int32, (lanes, n), 0)
    fill = jnp.zeros((lanes, n), F32)
    for t, f in enumerate(fill_terms()):
        fill = jnp.where(masked & (lane_row == e2 + t), f, fill)
    fill_col = jnp.transpose(fill)
    row_id = lax.broadcasted_iota(jnp.int32, (e, 2 * tj), 0)
    ones_rows = jnp.where(row_id < 3, 1.0, 0.0).astype(BF16)
    eye_r = lax.broadcasted_iota(jnp.int32, (tj, 2 * tj), 0)
    eye_c = lax.broadcasted_iota(jnp.int32, (tj, 2 * tj), 1)
    eye2 = jnp.where(eye_r == lax.rem(eye_c, tj), 1.0, 0.0).astype(BF16)
    z16 = jnp.zeros((e, tj), BF16)
    z_rows = jnp.zeros((lanes - 3 * e, 2 * tj), BF16)

    for d in order:
        x_copy(d, me_r, (me_r + rows - d) % rows).wait_recv()
    f_copy(0, me_c, mine).start()
    for d in y_order:
        y_copy(d, me_c).start()

    def wait_cols(jp):
        for d in order:
            a_copy(d, jp, me_r, (me_r + rows - d) % rows).wait_recv()

    def project(jp):
        a = a_ref[jp]
        r = mm_nt(w_qvg, a)
        q = (r[:proj2] * q_scale).astype(BF16)
        g = jax.nn.sigmoid(r[2 * proj2:])
        vt[jp] = r[proj2:2 * proj2].astype(BF16)
        for ib in range(cols):
            ls = slice(ib * tj, (ib + 1) * tj)
            gt[jp, ib] = g[:, ls]
            for h in range(heads):
                qp[jp, ib, h, 0:e, 0:tj] = q[h * e2:h * e2 + e, ls]
                qp[jp, ib, h, 0:e, tj:2 * tj] = z16
                qp[jp, ib, h, e:e2, 0:tj] = z16
                qp[jp, ib, h, e:e2, tj:2 * tj] = q[h * e2 + e:h * e2 + e2, ls]
                qp[jp, ib, h, e2:3 * e, :] = ones_rows
        k = mm_nt(a, w_kh)
        for h in range(heads):
            kh[jp, h] = (k[:, h * lanes:(h + 1) * lanes] + fill_col).astype(BF16)

    blk_a, blk_b, blk_d = (me_c + 1) % cols, (me_c + cols - 1) % cols, (me_c + 2) % cols

    halves = 2
    ck = n // halves
    slots = heads

    def scores_dot(ib, jp, h):
        rhs = jnp.concatenate([qp[jp, ib, h], z_rows, eye2], 0)
        return jnp.concatenate([mm(jnp.concatenate([kh[jp, h, c * ck:(c + 1) * ck], bias_ref[ib, h, c * ck:(c + 1) * ck]], 1), rhs) for c in range(halves)], 0)

    def drain(s, c, slot, mx):
        part = s[c * ck:(c + 1) * ck]
        ss[slot, c * ck:(c + 1) * ck] = part
        part = jnp.max(part.reshape(ck // 8, 8, 2 * tj), axis=0)
        return part if mx is None else jnp.maximum(mx, part)

    def weigh(jp, h, slot, c, l, o):
        rs = slice(c * ck, (c + 1) * ck)
        p = jnp.exp(ss[slot, rs] - mm_s[slot])
        part = jnp.sum(p.reshape(ck // 8, 8, 2 * tj), axis=0)
        ob = mm(vt[jp, h * e2:(h + 1) * e2, rs], p.astype(BF16))
        return (part, ob) if l is None else (l + part, o + ob)

    def scores(ib, jp, h):
        s = scores_dot(ib, jp, h)
        mx = None
        for c in range(halves):
            mx = drain(s, c, h, mx)
        mm_s[h] = jnp.max(mx, axis=0, keepdims=True)

    def finish_unit(jp, ib):
        parts = []
        for h in range(heads):
            l1 = jnp.sum(lp[h], axis=0, keepdims=True)
            for half in range(2):
                ls = slice(half * tj, (half + 1) * tj)
                rs = slice(h * e2 + half * e, h * e2 + (half + 1) * e)
                parts.append(gt[jp, ib, rs, :] * (os_[h, half * e:(half + 1) * e, ls] / l1[:, ls]))
        outb[jp, pl.ds(pl.multiple_of(ib * tj, tj), tj), :] = jnp.transpose(jnp.concatenate(parts, 0)).astype(BF16)

    def out_copy(dst_row, jp, count):
        rs, js = pl.ds(pl.multiple_of(dst_row * ti, ti), ti), pl.ds(jp, count)
        return remote(outb.at[js, rs, :], out_ref.at[me_r, js], o_sem.at[0, dst_row], o_sem.at[1, me_r], {'row': dst_row})

    def send_out(jp, ib, count=1):
        for k in range(per_blk):
            dst_row = ib * per_blk + k

            @pl.when(dst_row != me_r)
            def _():
                out_copy(dst_row, jp, count).start()

    def attend(jp, ib, jp_prev, ib_prev, jp_next, ib_next):
        finish_unit(jp_prev, ib_prev)
        for h in range(heads):
            nxt = (ib, jp, h + 2) if h + 2 < heads else (ib_next, jp_next, h + 2 - heads)
            s = scores_dot(*nxt)
            l, o, mx = None, None, None
            for c in range(halves):
                mx = drain(s, c, nxt[2], mx)
                l, o = weigh(jp, h, h, c, l, o)
            mm_s[nxt[2]] = jnp.max(mx, axis=0, keepdims=True)
            os_[h] = o
            lp[h] = l

    os_[...] = jnp.ones_like(os_)
    lp[...] = jnp.ones_like(lp)
    wait_cols(0)
    project(0)
    f_copy(0, me_c, other).wait_recv()
    for h in range(2):
        scores(me_c, 0, h)

    def bring(blk):
        d = (me_c - blk + cols) % cols
        y_copy(d, blk).wait_recv()
        f_copy(d, blk, mine).start()

    def relay(side, blk, step):
        part = pl.ds(core * hh + side * (hh // 2), hh // 2)
        return remote(bias_ref.at[blk, part], bias_ref.at[blk, part], g_sem.at[0, side], g_sem.at[1, side], {'col': (me_c + step) % cols})

    def brought(blk):
        f_copy((me_c - blk + cols) % cols, blk, other).wait_recv()

    def chain(units, prev, nxt):
        seq = [prev] + units + [nxt]
        for k in range(1, len(seq) - 1):
            attend(*seq[k], *seq[k - 1], *seq[k + 1])

    def pick(cond, yes, no):
        return tuple(jnp.where(cond, y, n) for y, n in zip(yes, no))

    n_a = hj // 2

    def lead_in(t, _):
        wait_cols(t + 1)
        project(t + 1)

        @pl.when(t == n_a - 1)
        def _():
            bring(blk_a)
            relay(0, blk_a, cols - 1).start()
            bring(blk_b)
            relay(1, blk_b, 1).start()

        chain([(t, me_c)], (jnp.maximum(t - 1, 0), me_c), (t + 1, me_c))
        return 0

    lax.fori_loop(0, n_a, lead_in, 0)
    brought(blk_a)
    brought(blk_b)

    def role(offsets):
        return (me_c + sum(jnp.where(shift == k, o, 0) for k, o in enumerate(offsets))) % cols

    shift = (chip - me_c + cols) % cols
    odd = chip % 2
    blk_p, blk_q, blk_r = role((1 + 2 * odd, 3, 1, 1)), role((2, 2, 3, 2)), role((3 - 2 * odd, 1, 2, 3))

    def late(w):
        own = shift == 0
        jp = jnp.where(w < 0, w + hj, jnp.where(own, 2 * (w // 4) + w % 2, w % hj))
        second = jnp.where(own, (w // 2) % 2, w // hj)
        return jp, jnp.where(w < 0, blk_p, jnp.where(second == 0, blk_q, blk_r))

    def send_earlier(t):
        k = 2 * (t - n_a)

        @pl.when(t == n_a + 1)
        def _():
            send_out(0, me_c, n_a)

        @pl.when(t > n_a + 1)
        def _():
            send_out(k - 4, blk_p, 2)

    def three(t, _):
        wait_cols(t + 1)
        project(t + 1)
        k = 2 * (t - n_a)
        chain([(t, me_c), (k, blk_p), (k + 1, blk_p)], pick(t == n_a, (t - 1, me_c), (k - 1, blk_p)), (t + 1, me_c))
        return 0

    lax.fori_loop(n_a, hj - 1, three, 0)
    relay(0, blk_d, cols - 1).wait_recv()
    relay(1, blk_d, 1).wait_recv()
    f_copy(2, blk_d, mine).start()

    def bridge(t, _):
        send_out(0, me_c, n_a)
        send_out(0, blk_p, n_a)
        k = 2 * (t - n_a)
        chain([(t, me_c), (k, blk_p), (k + 1, blk_p)], (k - 1, blk_p), (0, blk_q))
        return 0

    brought(blk_d)
    lax.fori_loop(hj - 1, hj, bridge, 0)

    def four(s, _):
        @pl.when(s == 0)
        def _():
            send_out(n_a, me_c, n_a)
            send_out(hj - 4, blk_p, 2)

        @pl.when(s > 0)
        def _():
            send_out(*late(4 * s - 6), 2)
            send_out(*late(4 * s - 4), 2)

        chain([late(4 * s + k) for k in range(4)], late(4 * s - 1), late(jnp.minimum(4 * s + 4, 2 * hj - 1)))
        return 0

    lax.fori_loop(0, hj // 2, four, 0)
    send_out(*late(2 * hj - 6), 2)
    send_out(*late(2 * hj - 4), 2)
    finish_unit(*late(2 * hj - 1))
    send_out(*late(2 * hj - 2), 2)
    own = pltpu.make_async_copy(outb.at[:, my_rows, :], out_ref.at[me_r], l_sem)
    own.start()

    for d in order:
        x_copy(d, (me_r + d) % rows, me_r).wait_send()
        for jp in range(hj):
            a_copy(d, jp, (me_r + d) % rows, me_r).wait_send()
    for d in y_order:
        y_copy(d, me_c).wait_send()
    relay(0, blk_a, cols - 1).wait_send()
    relay(1, blk_b, 1).wait_send()
    for d in range(cols):
        f_copy(d, me_c, mine).wait_send()

    def all_out(send_row, slot):
        rs = pl.ds(pl.multiple_of(send_row * ti, ti), ti)
        return remote(outb.at[:, rs, :], out_ref.at[slot], o_sem.at[0, send_row], o_sem.at[1, slot], {'row': partner})

    for d in order:
        src = (me_r + rows - d) % rows
        all_out(src, src).wait_recv()
    own.wait()
    for d in order:
        dst = (me_r + d) % rows
        all_out(dst, dst).wait_send()


def finish_kernel(e, g_ref, z_ref, wo_ref, out_ref, stage):
    rows, hj, ti, lanes = g_ref.shape
    ch, tj = z_ref.shape[1:]
    pitch = ti + PAD
    n_rj = rows * hj
    wo = wo_ref[...].astype(F32)
    z = jnp.zeros((e, ch), F32)
    wo = tr(jnp.concatenate([blk for r in range(0, wo.shape[0], e) for blk in (wo[r:r + e], z)], 0))
    for rj in range(n_rj):
        stage[rj * pitch:rj * pitch + ti, :] = g_ref[rj // hj, rj % hj].astype(F32)
    for i in range(ti):
        x = stage[pl.ds(i, n_rj, stride=pitch), :]
        y = pltpu.roll(x, lanes - e, 1)
        x2 = jnp.concatenate([x.reshape(rows, 1, hj, lanes), y.reshape(rows, 1, hj, lanes)], 1).reshape(tj, lanes).astype(BF16)
        out_ref[i] = (mm_nt(wo, x2) + z_ref[i].astype(F32)).astype(BF16)


VM = pl.BlockSpec(memory_space=pltpu.VMEM)


def solution(mesh):
    rows, cols = mesh.shape['row'], mesh.shape['col']

    def body(pair_tile, res_mask, ln_gamma, ln_beta, w_q, w_k, w_v, w_b, w_g, w_o):
        ti, tj, ch = pair_tile.shape
        heads = w_b.shape[1]
        proj = w_q.shape[1]
        n = ti * rows
        hj = tj // rows // 2
        z = jnp.transpose(pair_tile, (0, 2, 1))
        dma = pltpu.SemaphoreType.DMA
        e = proj // heads
        back = pl.pallas_call(
            functools.partial(triangle_kernel, rows, cols),
            out_shape=jax.ShapeDtypeStruct((rows, hj, ti, 2 * ch), BF16),
            in_specs=[VM] * 9,
            out_specs=pl.BlockSpec(memory_space=pl.ANY),
            scratch_shapes=[
                pltpu.VMEM((ti * (rows * hj + PAD), 2 * ch), F32),
                pltpu.VMEM((ti * heads, tj), F32),
                pltpu.VMEM((heads, ti, tj), BF16),
                pltpu.VMEM((rows, hj, ti, 2 * ch), BF16),
                pltpu.VMEM((hj, n, 2 * ch), BF16),
                pltpu.VMEM((cols, heads, n, tj), BF16),
                pltpu.VMEM((hj, cols, heads, 3 * e, 2 * tj), BF16),
                pltpu.VMEM((hj, 2 * proj, n), BF16),
                pltpu.VMEM((hj, cols, 2 * proj, tj), F32),
                pltpu.VMEM((hj, heads, n, 2 * ch), BF16),
                pltpu.VMEM((heads, n, 2 * tj), F32),
                pltpu.VMEM((heads, 1, 2 * tj), F32),
                pltpu.VMEM((heads, 8, 2 * tj), F32),
                pltpu.VMEM((heads, 2 * e, 2 * tj), F32),
                pltpu.VMEM((hj, n, 2 * proj), BF16),
                dma((2, hj, rows)), dma((2, rows)), dma((2, cols)), dma((2, cols)), dma((2, 2)), dma((2, rows)), dma,
            ],
            compiler_params=pltpu.CompilerParams(collective_id=0, has_side_effects=True),
            name='triangle',
        )(z, ln_gamma.reshape(1, ch), ln_beta.reshape(1, ch), w_b.T, res_mask.reshape(1, n), w_q, w_k, w_v, w_g)
        chunk = ti // 2
        out = pl.pallas_call(
            functools.partial(finish_kernel, proj // heads),
            out_shape=jax.ShapeDtypeStruct((ti, ch, tj), BF16),
            grid=(ti // chunk,),
            in_specs=[
                pl.BlockSpec((rows, hj, chunk, 2 * ch), lambda i: (0, 0, i, 0)),
                pl.BlockSpec((chunk, ch, tj), lambda i: (i, 0, 0)),
                pl.BlockSpec((proj, ch), lambda i: (0, 0)),
            ],
            out_specs=pl.BlockSpec((chunk, ch, tj), lambda i: (i, 0, 0)),
            scratch_shapes=[pltpu.VMEM((rows * hj * (chunk + PAD), 2 * ch), F32)],
            name='finish',
        )(back, z, w_o)
        return jnp.transpose(out, (0, 2, 1))

    tile_spec = P(('data', 'row'), 'col', None)
    return jax.shard_map(body, mesh=mesh, in_specs=(tile_spec, P('data'), P(), P(), P(), P(), P(), P(), P(), P()), out_specs=tile_spec, check_vma=False)
```

```python
import functools
import math

import jax
import jax.numpy as jnp
import numpy as np
from jax import lax
from jax.experimental import pallas as pl
from jax.experimental.pallas import tpu as pltpu
from jax.sharding import PartitionSpec as P

LN_EPS = 1e-5
MASK_FILL = -1e9
MESH = pl.DeviceIdType.MESH
F32, BF16 = jnp.float32, jnp.bfloat16
NT = (((1,), (1,)), ((), ()))
PAD = 8


def mm(a, b):
    return jnp.dot(a, b, preferred_element_type=F32)


def mm_nt(a, b):
    return lax.dot_general(a, b, NT, preferred_element_type=F32)


def tr(w):
    return jnp.transpose(w.astype(F32)).astype(BF16)


def block_diag2(w):
    z = jnp.zeros_like(w)
    return jnp.concatenate([jnp.concatenate([w, z], 1), jnp.concatenate([z, w], 1)], 0)


def remote(src, dst, send, recv, dev):
    return pltpu.make_async_remote_copy(src_ref=src, dst_ref=dst, send_sem=send, recv_sem=recv, device_id=dev, device_id_type=MESH)


def fill_terms():
    rest, terms = MASK_FILL, []
    for _ in range(3):
        t = float(np.asarray(rest, dtype=BF16))
        terms.append(t)
        rest -= t
    return terms


def pair_rows(wt, e):
    z = jnp.zeros_like(wt)
    lo, hi = jnp.concatenate([wt, z], 1), jnp.concatenate([z, wt], 1)
    return [blk for r in range(0, wt.shape[0], e) for blk in (lo[r:r + e], hi[r:r + e])]


def triangle_kernel(rows, cols, z_ref, gamma_ref, beta_ref, wb_ref, mask_ref, wq_ref, wk_ref, wv_ref, wg_ref, out_ref,
                    stage, bsc, bown, send, a_ref, bias_ref, qp, vt, gt, kh, ss, mm_s, lp, os_, outb, a_sem, x_sem, y_sem, f_sem, g_sem, o_sem, l_sem):
    ti, ch, tj = z_ref.shape
    heads = wb_ref.shape[0]
    hj, n, lanes = a_ref.shape
    e = wq_ref.shape[1] // heads
    e2 = 2 * e
    proj2 = 2 * heads * e
    q_scale = 1.0 / math.sqrt(e)
    pitch = rows * hj + PAD
    per_blk = tj // ti
    me_r, me_c = lax.axis_index('row'), lax.axis_index('col')
    core = me_r % 2
    partner = me_r + 1 - 2 * core
    chip = me_r // 2

    barrier = pltpu.get_barrier_semaphore()
    for d in range(1, rows):
        pl.semaphore_signal(barrier, inc=1, device_id={'row': (me_r + d) % rows}, device_id_type=MESH)
    for d in range(1, cols):
        pl.semaphore_signal(barrier, inc=1, device_id={'col': (me_c + d) % cols}, device_id_type=MESH)

    gam = jnp.transpose(jnp.broadcast_to(gamma_ref[...], (tj, ch)))
    bet = jnp.transpose(jnp.broadcast_to(beta_ref[...], (tj, ch)))
    group = 4
    wb = wb_ref[...].astype(F32)
    wb16 = jnp.concatenate([wb] * group, 0)
    wb16 = jnp.concatenate([wb16] * group, 1)
    r_id = lax.broadcasted_iota(jnp.int32, wb16.shape, 0) // heads
    c_id = lax.broadcasted_iota(jnp.int32, wb16.shape, 1) // ch
    wb16 = jnp.where(r_id == c_id, wb16, 0.0).astype(BF16)
    unroll = 16

    def norm_step(t, _):
        for u in range(unroll):
            i0 = (t * unroll + u) * group
            x = z_ref[pl.ds(i0, group)].astype(F32)
            mean = jnp.sum(x, axis=1, keepdims=True) * (1.0 / ch)
            cen = x - mean
            var = jnp.sum(cen * cen, axis=1, keepdims=True) * (1.0 / ch)
            nrm = cen * lax.rsqrt(var + LN_EPS) * gam + bet
            bsc[pl.ds(pl.multiple_of(i0 * heads, group * heads), group * heads), :] = mm(wb16, nrm.astype(BF16).reshape(group * ch, tj))
            for q in range(group):
                t4 = jnp.transpose(nrm[q]).reshape(rows, 2, hj, ch)
                packed = jnp.concatenate([t4[:, 0], t4[:, 1]], axis=-1).reshape(rows * hj, 2 * ch)
                stage[pl.ds(pl.multiple_of((i0 + q) * pitch, 8), rows * hj), :] = packed
        return 0

    lax.fori_loop(0, ti // group // unroll, norm_step, 0)

    my_rows = pl.ds(pl.multiple_of(me_r * ti, ti), ti)
    hh = heads // 2
    mine, other = pl.ds(core * hh, hh), pl.ds((1 - core) * hh, hh)
    for h in range(heads):
        bown[h] = bsc[pl.ds(h, ti, stride=heads), :].astype(BF16)
    bias_ref[me_c, mine, my_rows, :] = bown[mine]

    def x_copy(d, dst_row, src_row):
        rs = pl.ds(pl.multiple_of(src_row * ti, ti), ti)
        part = pl.ds((dst_row % 2) * hh, hh)
        return remote(bown.at[part], bias_ref.at[me_c, part, rs, :], x_sem.at[0, d], x_sem.at[1, d], {'row': (me_r + d) % rows})

    def a_copy(d, jp, dst_row, src_row):
        rs = pl.ds(pl.multiple_of(src_row * ti, ti), ti)
        return remote(send.at[dst_row, jp], a_ref.at[jp, rs, :], a_sem.at[0, jp, d], a_sem.at[1, jp, d], {'row': (me_r + d) % rows})

    def piece(dst_row, jp):
        return stage[pl.ds(dst_row * hj + jp, ti, stride=pitch), :].astype(BF16)

    def y_copy(d, blk):
        return remote(bias_ref.at[blk, mine], bias_ref.at[blk, mine], y_sem.at[0, d], y_sem.at[1, d], {'col': (me_c + d) % cols})

    def f_copy(d, blk, part):
        return remote(bias_ref.at[blk, part], bias_ref.at[blk, part], f_sem.at[0, d], f_sem.at[1, d], {'row': partner})

    order = [4, 3, 5, 2, 6, 1, 7] if rows == 8 else list(range(1, rows))
    y_order = [1, cols - 1]

    pl.semaphore_wait(barrier, rows + cols - 2)
    for d in order:
        x_copy(d, (me_r + d) % rows, me_r).start()
    for jp in range(hj + 1):
        if jp < hj:
            for d in order:
                dst = (me_r + d) % rows
                send[dst, jp] = piece(dst, jp)
            a_ref[jp, my_rows, :] = piece(me_r, jp)
        if jp > 0:
            for d in order:
                a_copy(d, jp - 1, (me_r + d) % rows, me_r).start()

    w_qvg = jnp.concatenate(pair_rows(tr(wq_ref[...]), e) + pair_rows(tr(wv_ref[...]), e) + pair_rows(tr(wg_ref[...]), e), 0)
    k_rows = pair_rows(tr(wk_ref[...]), e)
    k_pad = jnp.zeros((lanes - e2, lanes), BF16)
    w_kh = jnp.concatenate([b for h in range(heads) for b in (k_rows[2 * h], k_rows[2 * h + 1], k_pad)], 0)
    masked = jnp.broadcast_to(mask_ref[...] == 0, (lanes, n))
    lane_row = lax.broadcasted_iota(jnp.int32, (lanes, n), 0)
    fill = jnp.zeros((lanes, n), F32)
    for t, f in enumerate(fill_terms()):
        fill = jnp.where(masked & (lane_row == e2 + t), f, fill)
    fill_col = jnp.transpose(fill)
    row_id = lax.broadcasted_iota(jnp.int32, (e, 2 * tj), 0)
    ones_rows = jnp.where(row_id < 3, 1.0, 0.0).astype(BF16)
    eye_r = lax.broadcasted_iota(jnp.int32, (tj, 2 * tj), 0)
    eye_c = lax.broadcasted_iota(jnp.int32, (tj, 2 * tj), 1)
    eye2 = jnp.where(eye_r == lax.rem(eye_c, tj), 1.0, 0.0).astype(BF16)
    z16 = jnp.zeros((e, tj), BF16)
    z_rows = jnp.zeros((lanes - 3 * e, 2 * tj), BF16)

    for d in order:
        x_copy(d, me_r, (me_r + rows - d) % rows).wait_recv()
    f_copy(0, me_c, mine).start()
    for d in y_order:
        y_copy(d, me_c).start()

    def wait_cols(jp):
        for d in order:
            a_copy(d, jp, me_r, (me_r + rows - d) % rows).wait_recv()

    def project(jp):
        a = a_ref[jp]
        r = mm_nt(w_qvg, a)
        q = (r[:proj2] * q_scale).astype(BF16)
        g = jax.nn.sigmoid(r[2 * proj2:])
        vt[jp] = r[proj2:2 * proj2].astype(BF16)
        for ib in range(cols):
            ls = slice(ib * tj, (ib + 1) * tj)
            gt[jp, ib] = g[:, ls]
            for h in range(heads):
                qp[jp, ib, h, 0:e, 0:tj] = q[h * e2:h * e2 + e, ls]
                qp[jp, ib, h, 0:e, tj:2 * tj] = z16
                qp[jp, ib, h, e:e2, 0:tj] = z16
                qp[jp, ib, h, e:e2, tj:2 * tj] = q[h * e2 + e:h * e2 + e2, ls]
                qp[jp, ib, h, e2:3 * e, :] = ones_rows
        k = mm_nt(a, w_kh)
        for h in range(heads):
            kh[jp, h] = (k[:, h * lanes:(h + 1) * lanes] + fill_col).astype(BF16)

    blk_a, blk_b, blk_d = (me_c + 1) % cols, (me_c + cols - 1) % cols, (me_c + 2) % cols

    halves = 2
    ck = n // halves
    slots = heads

    def scores_dot(ib, jp, h):
        rhs = jnp.concatenate([qp[jp, ib, h], z_rows, eye2], 0)
        return jnp.concatenate([mm(jnp.concatenate([kh[jp, h, c * ck:(c + 1) * ck], bias_ref[ib, h, c * ck:(c + 1) * ck]], 1), rhs) for c in range(halves)], 0)

    def drain(s, c, slot, mx):
        part = s[c * ck:(c + 1) * ck]
        ss[slot, c * ck:(c + 1) * ck] = part
        part = jnp.max(part.reshape(ck // 8, 8, 2 * tj), axis=0)
        return part if mx is None else jnp.maximum(mx, part)

    def weigh(jp, h, slot, c, l, o):
        rs = slice(c * ck, (c + 1) * ck)
        p = jnp.exp(ss[slot, rs] - mm_s[slot])
        part = jnp.sum(p.reshape(ck // 8, 8, 2 * tj), axis=0)
        ob = mm(vt[jp, h * e2:(h + 1) * e2, rs], p.astype(BF16))
        return (part, ob) if l is None else (l + part, o + ob)

    def scores(ib, jp, h):
        s = scores_dot(ib, jp, h)
        mx = None
        for c in range(halves):
            mx = drain(s, c, h, mx)
        mm_s[h] = jnp.max(mx, axis=0, keepdims=True)

    def finish_unit(jp, ib):
        parts = []
        for h in range(heads):
            l1 = jnp.sum(lp[h], axis=0, keepdims=True)
            for half in range(2):
                ls = slice(half * tj, (half + 1) * tj)
                rs = slice(h * e2 + half * e, h * e2 + (half + 1) * e)
                parts.append(gt[jp, ib, rs, :] * (os_[h, half * e:(half + 1) * e, ls] / l1[:, ls]))
        outb[jp, pl.ds(pl.multiple_of(ib * tj, tj), tj), :] = jnp.transpose(jnp.concatenate(parts, 0)).astype(BF16)

    def out_copy(dst_row, jp, count):
        rs, js = pl.ds(pl.multiple_of(dst_row * ti, ti), ti), pl.ds(jp, count)
        return remote(outb.at[js, rs, :], out_ref.at[me_r, js], o_sem.at[0, dst_row], o_sem.at[1, me_r], {'row': dst_row})

    def send_out(jp, ib, count=1):
        for k in range(per_blk):
            dst_row = ib * per_blk + k

            @pl.when(dst_row != me_r)
            def _():
                out_copy(dst_row, jp, count).start()

    def attend(jp, ib, jp_prev, ib_prev, jp_next, ib_next):
        finish_unit(jp_prev, ib_prev)
        for h in range(heads):
            nxt = (ib, jp, h + 2) if h + 2 < heads else (ib_next, jp_next, h + 2 - heads)
            s = scores_dot(*nxt)
            l, o, mx = None, None, None
            for c in range(halves):
                mx = drain(s, c, nxt[2], mx)
                l, o = weigh(jp, h, h, c, l, o)
            mm_s[nxt[2]] = jnp.max(mx, axis=0, keepdims=True)
            os_[h] = o
            lp[h] = l

    os_[...] = jnp.ones_like(os_)
    lp[...] = jnp.ones_like(lp)
    wait_cols(0)
    project(0)
    f_copy(0, me_c, other).wait_recv()
    for h in range(2):
        scores(me_c, 0, h)

    def bring(blk):
        d = (me_c - blk + cols) % cols
        y_copy(d, blk).wait_recv()
        f_copy(d, blk, mine).start()

    def relay(side, blk, step):
        part = pl.ds(core * hh + side * (hh // 2), hh // 2)
        return remote(bias_ref.at[blk, part], bias_ref.at[blk, part], g_sem.at[0, side], g_sem.at[1, side], {'col': (me_c + step) % cols})

    def brought(blk):
        f_copy((me_c - blk + cols) % cols, blk, other).wait_recv()

    def chain(units, prev, nxt):
        seq = [prev] + units + [nxt]
        for k in range(1, len(seq) - 1):
            attend(*seq[k], *seq[k - 1], *seq[k + 1])

    def pick(cond, yes, no):
        return tuple(jnp.where(cond, y, n) for y, n in zip(yes, no))

    n_a = hj // 2

    def lead_in(t, _):
        wait_cols(t + 1)
        project(t + 1)

        @pl.when(t == n_a - 1)
        def _():
            bring(blk_a)
            relay(0, blk_a, cols - 1).start()
            bring(blk_b)
            relay(1, blk_b, 1).start()

        chain([(t, me_c)], (jnp.maximum(t - 1, 0), me_c), (t + 1, me_c))
        return 0

    lax.fori_loop(0, n_a, lead_in, 0)
    brought(blk_a)
    brought(blk_b)

    def role(offsets):
        return (me_c + sum(jnp.where(shift == k, o, 0) for k, o in enumerate(offsets))) % cols

    shift = (chip - me_c + cols) % cols
    odd = chip % 2
    blk_p, blk_q, blk_r = role((1 + 2 * odd, 3, 1, 1)), role((2, 2, 3, 2)), role((3 - 2 * odd, 1, 2, 3))

    def late(w):
        own = shift == 0
        jp = jnp.where(w < 0, w + hj, jnp.where(own, 2 * (w // 4) + w % 2, w % hj))
        second = jnp.where(own, (w // 2) % 2, w // hj)
        return jp, jnp.where(w < 0, blk_p, jnp.where(second == 0, blk_q, blk_r))

    def send_earlier(t):
        k = 2 * (t - n_a)

        @pl.when(t == n_a + 1)
        def _():
            send_out(0, me_c, n_a)

        @pl.when(t > n_a + 1)
        def _():
            send_out(k - 4, blk_p, 2)

    def three(t, _):
        wait_cols(t + 1)
        project(t + 1)
        k = 2 * (t - n_a)
        chain([(t, me_c), (k, blk_p), (k + 1, blk_p)], pick(t == n_a, (t - 1, me_c), (k - 1, blk_p)), (t + 1, me_c))
        return 0

    lax.fori_loop(n_a, hj - 1, three, 0)
    relay(0, blk_d, cols - 1).wait_recv()
    relay(1, blk_d, 1).wait_recv()
    f_copy(2, blk_d, mine).start()

    def bridge(t, _):
        send_out(0, me_c, n_a)
        send_out(0, blk_p, n_a)
        k = 2 * (t - n_a)
        chain([(t, me_c), (k, blk_p), (k + 1, blk_p)], (k - 1, blk_p), (0, blk_q))
        return 0

    brought(blk_d)
    lax.fori_loop(hj - 1, hj, bridge, 0)

    def four(s, _):
        @pl.when(s == 0)
        def _():
            send_out(n_a, me_c, n_a)
            send_out(hj - 4, blk_p, 2)

        @pl.when(s > 0)
        def _():
            send_out(*late(4 * s - 6), 2)
            send_out(*late(4 * s - 4), 2)

        chain([late(4 * s + k) for k in range(4)], late(4 * s - 1), late(jnp.minimum(4 * s + 4, 2 * hj - 1)))
        return 0

    lax.fori_loop(0, hj // 2, four, 0)
    send_out(*late(2 * hj - 6), 2)
    send_out(*late(2 * hj - 4), 2)
    finish_unit(*late(2 * hj - 1))
    send_out(*late(2 * hj - 2), 2)
    own = pltpu.make_async_copy(outb.at[:, my_rows, :], out_ref.at[me_r], l_sem)
    own.start()

    for d in order:
        x_copy(d, (me_r + d) % rows, me_r).wait_send()
        for jp in range(hj):
            a_copy(d, jp, (me_r + d) % rows, me_r).wait_send()
    for d in y_order:
        y_copy(d, me_c).wait_send()
    relay(0, blk_a, cols - 1).wait_send()
    relay(1, blk_b, 1).wait_send()
    for d in range(cols):
        f_copy(d, me_c, mine).wait_send()

    def all_out(send_row, slot):
        rs = pl.ds(pl.multiple_of(send_row * ti, ti), ti)
        return remote(outb.at[:, rs, :], out_ref.at[slot], o_sem.at[0, send_row], o_sem.at[1, slot], {'row': partner})

    for d in order:
        src = (me_r + rows - d) % rows
        all_out(src, src).wait_recv()
    own.wait()
    for d in order:
        dst = (me_r + d) % rows
        all_out(dst, dst).wait_send()


def finish_kernel(e, g_ref, z_ref, wo_ref, out_ref, stage):
    rows, hj, ti, lanes = g_ref.shape
    ch, tj = z_ref.shape[1:]
    pitch = ti + PAD
    n_rj = rows * hj
    wo = wo_ref[...].astype(F32)
    z = jnp.zeros((e, ch), F32)
    wo = tr(jnp.concatenate([blk for r in range(0, wo.shape[0], e) for blk in (wo[r:r + e], z)], 0))
    for rj in range(n_rj):
        stage[rj * pitch:rj * pitch + ti, :] = g_ref[rj // hj, rj % hj].astype(F32)
    def columns(i):
        x = stage[pl.ds(i, n_rj, stride=pitch), :]
        y = pltpu.roll(x, lanes - e, 1)
        return jnp.concatenate([x.reshape(rows, 1, hj, lanes), y.reshape(rows, 1, hj, lanes)], 1).reshape(tj, lanes).astype(BF16)

    for i in range(0, ti, 2):
        r = mm_nt(wo, jnp.concatenate([columns(i), columns(i + 1)], 0))
        out_ref[i] = (r[:, :tj] + z_ref[i].astype(F32)).astype(BF16)
        out_ref[i + 1] = (r[:, tj:] + z_ref[i + 1].astype(F32)).astype(BF16)


VM = pl.BlockSpec(memory_space=pltpu.VMEM)


def solution(mesh):
    rows, cols = mesh.shape['row'], mesh.shape['col']

    def body(pair_tile, res_mask, ln_gamma, ln_beta, w_q, w_k, w_v, w_b, w_g, w_o):
        ti, tj, ch = pair_tile.shape
        heads = w_b.shape[1]
        proj = w_q.shape[1]
        n = ti * rows
        hj = tj // rows // 2
        z = jnp.transpose(pair_tile, (0, 2, 1))
        dma = pltpu.SemaphoreType.DMA
        e = proj // heads
        back = pl.pallas_call(
            functools.partial(triangle_kernel, rows, cols),
            out_shape=jax.ShapeDtypeStruct((rows, hj, ti, 2 * ch), BF16),
            in_specs=[VM] * 9,
            out_specs=pl.BlockSpec(memory_space=pl.ANY),
            scratch_shapes=[
                pltpu.VMEM((ti * (rows * hj + PAD), 2 * ch), F32),
                pltpu.VMEM((ti * heads, tj), F32),
                pltpu.VMEM((heads, ti, tj), BF16),
                pltpu.VMEM((rows, hj, ti, 2 * ch), BF16),
                pltpu.VMEM((hj, n, 2 * ch), BF16),
                pltpu.VMEM((cols, heads, n, tj), BF16),
                pltpu.VMEM((hj, cols, heads, 3 * e, 2 * tj), BF16),
                pltpu.VMEM((hj, 2 * proj, n), BF16),
                pltpu.VMEM((hj, cols, 2 * proj, tj), F32),
                pltpu.VMEM((hj, heads, n, 2 * ch), BF16),
                pltpu.VMEM((heads, n, 2 * tj), F32),
                pltpu.VMEM((heads, 1, 2 * tj), F32),
                pltpu.VMEM((heads, 8, 2 * tj), F32),
                pltpu.VMEM((heads, 2 * e, 2 * tj), F32),
                pltpu.VMEM((hj, n, 2 * proj), BF16),
                dma((2, hj, rows)), dma((2, rows)), dma((2, cols)), dma((2, cols)), dma((2, 2)), dma((2, rows)), dma,
            ],
            compiler_params=pltpu.CompilerParams(collective_id=0, has_side_effects=True),
            name='triangle',
        )(z, ln_gamma.reshape(1, ch), ln_beta.reshape(1, ch), w_b.T, res_mask.reshape(1, n), w_q, w_k, w_v, w_g)
        chunk = ti // 2
        out = pl.pallas_call(
            functools.partial(finish_kernel, proj // heads),
            out_shape=jax.ShapeDtypeStruct((ti, ch, tj), BF16),
            grid=(ti // chunk,),
            in_specs=[
                pl.BlockSpec((rows, hj, chunk, 2 * ch), lambda i: (0, 0, i, 0)),
                pl.BlockSpec((chunk, ch, tj), lambda i: (i, 0, 0)),
                pl.BlockSpec((proj, ch), lambda i: (0, 0)),
            ],
            out_specs=pl.BlockSpec((chunk, ch, tj), lambda i: (i, 0, 0)),
            scratch_shapes=[pltpu.VMEM((rows * hj * (chunk + PAD), 2 * ch), F32)],
            name='finish',
        )(back, z, w_o)
        return jnp.transpose(out, (0, 2, 1))

    tile_spec = P(('data', 'row'), 'col', None)
    return jax.shard_map(body, mesh=mesh, in_specs=(tile_spec, P('data'), P(), P(), P(), P(), P(), P(), P(), P()), out_specs=tile_spec, check_vma=False)
```

```python
import functools
import math

import jax
import jax.numpy as jnp
import numpy as np
from jax import lax
from jax.experimental import pallas as pl
from jax.experimental.pallas import tpu as pltpu
from jax.sharding import PartitionSpec as P

LN_EPS = 1e-5
MASK_FILL = -1e9
MESH = pl.DeviceIdType.MESH
F32, BF16 = jnp.float32, jnp.bfloat16
NT = (((1,), (1,)), ((), ()))
PAD = 8


def mm(a, b):
    return jnp.dot(a, b, preferred_element_type=F32)


def mm_nt(a, b):
    return lax.dot_general(a, b, NT, preferred_element_type=F32)


def tr(w):
    return jnp.transpose(w.astype(F32)).astype(BF16)


def block_diag2(w):
    z = jnp.zeros_like(w)
    return jnp.concatenate([jnp.concatenate([w, z], 1), jnp.concatenate([z, w], 1)], 0)


def remote(src, dst, send, recv, dev):
    return pltpu.make_async_remote_copy(src_ref=src, dst_ref=dst, send_sem=send, recv_sem=recv, device_id=dev, device_id_type=MESH)


def fill_terms():
    rest, terms = MASK_FILL, []
    for _ in range(3):
        t = float(np.asarray(rest, dtype=BF16))
        terms.append(t)
        rest -= t
    return terms


def pair_rows(wt, e):
    z = jnp.zeros_like(wt)
    lo, hi = jnp.concatenate([wt, z], 1), jnp.concatenate([z, wt], 1)
    return [blk for r in range(0, wt.shape[0], e) for blk in (lo[r:r + e], hi[r:r + e])]


def triangle_kernel(rows, cols, z_ref, gamma_ref, beta_ref, wb_ref, mask_ref, wq_ref, wk_ref, wv_ref, wg_ref, out_ref,
                    stage, bsc, bown, send, a_ref, bias_ref, qp, vt, gt, kh, ss, mm_s, lp, os_, outb, a_sem, x_sem, y_sem, f_sem, g_sem, o_sem, l_sem):
    ti, ch, tj = z_ref.shape
    heads = wb_ref.shape[0]
    hj, n, lanes = a_ref.shape
    e = wq_ref.shape[1] // heads
    e2 = 2 * e
    proj2 = 2 * heads * e
    q_scale = 1.0 / math.sqrt(e)
    pitch = rows * hj + PAD
    per_blk = tj // ti
    me_r, me_c = lax.axis_index('row'), lax.axis_index('col')
    core = me_r % 2
    partner = me_r + 1 - 2 * core
    chip = me_r // 2

    barrier = pltpu.get_barrier_semaphore()
    for d in range(1, rows):
        pl.semaphore_signal(barrier, inc=1, device_id={'row': (me_r + d) % rows}, device_id_type=MESH)
    for d in range(1, cols):
        pl.semaphore_signal(barrier, inc=1, device_id={'col': (me_c + d) % cols}, device_id_type=MESH)

    gam = jnp.transpose(jnp.broadcast_to(gamma_ref[...], (tj, ch)))
    bet = jnp.transpose(jnp.broadcast_to(beta_ref[...], (tj, ch)))
    group = 4
    wb = wb_ref[...].astype(F32)
    wb16 = jnp.concatenate([wb] * group, 0)
    wb16 = jnp.concatenate([wb16] * group, 1)
    r_id = lax.broadcasted_iota(jnp.int32, wb16.shape, 0) // heads
    c_id = lax.broadcasted_iota(jnp.int32, wb16.shape, 1) // ch
    wb16 = jnp.where(r_id == c_id, wb16, 0.0).astype(BF16)
    unroll = 16

    def norm_step(t, _):
        for u in range(unroll):
            i0 = (t * unroll + u) * group
            x = z_ref[pl.ds(i0, group)].astype(F32)
            mean = jnp.sum(x, axis=1, keepdims=True) * (1.0 / ch)
            cen = x - mean
            var = jnp.sum(cen * cen, axis=1, keepdims=True) * (1.0 / ch)
            nrm = cen * lax.rsqrt(var + LN_EPS) * gam + bet
            bsc[pl.ds(pl.multiple_of(i0 * heads, group * heads), group * heads), :] = mm(wb16, nrm.astype(BF16).reshape(group * ch, tj))
            for q in range(group):
                t4 = jnp.transpose(nrm[q]).reshape(rows, 2, hj, ch)
                packed = jnp.concatenate([t4[:, 0], t4[:, 1]], axis=-1).reshape(rows * hj, 2 * ch)
                stage[pl.ds(pl.multiple_of((i0 + q) * pitch, 8), rows * hj), :] = packed
        return 0

    lax.fori_loop(0, ti // group // unroll, norm_step, 0)

    my_rows = pl.ds(pl.multiple_of(me_r * ti, ti), ti)
    hh = heads // 2
    mine, other = pl.ds(core * hh, hh), pl.ds((1 - core) * hh, hh)
    for h in range(heads):
        bown[h] = bsc[pl.ds(h, ti, stride=heads), :].astype(BF16)
    bias_ref[me_c, mine, my_rows, :] = bown[mine]

    def x_copy(d, dst_row, src_row):
        rs = pl.ds(pl.multiple_of(src_row * ti, ti), ti)
        part = pl.ds((dst_row % 2) * hh, hh)
        return remote(bown.at[part], bias_ref.at[me_c, part, rs, :], x_sem.at[0, d], x_sem.at[1, d], {'row': (me_r + d) % rows})

    def a_copy(d, jp, dst_row, src_row):
        rs = pl.ds(pl.multiple_of(src_row * ti, ti), ti)
        return remote(send.at[dst_row, jp], a_ref.at[jp, rs, :], a_sem.at[0, jp, d], a_sem.at[1, jp, d], {'row': (me_r + d) % rows})

    def piece(dst_row, jp):
        return stage[pl.ds(dst_row * hj + jp, ti, stride=pitch), :].astype(BF16)

    def y_copy(d, blk):
        return remote(bias_ref.at[blk, mine], bias_ref.at[blk, mine], y_sem.at[0, d], y_sem.at[1, d], {'col': (me_c + d) % cols})

    def f_copy(d, blk, part):
        return remote(bias_ref.at[blk, part], bias_ref.at[blk, part], f_sem.at[0, d], f_sem.at[1, d], {'row': partner})

    order = [4, 3, 5, 2, 6, 1, 7] if rows == 8 else list(range(1, rows))
    y_order = [1, cols - 1]

    pl.semaphore_wait(barrier, rows + cols - 2)
    for d in order:
        x_copy(d, (me_r + d) % rows, me_r).start()
    for jp in range(hj + 1):
        if jp < hj:
            for d in order:
                dst = (me_r + d) % rows
                send[dst, jp] = piece(dst, jp)
            a_ref[jp, my_rows, :] = piece(me_r, jp)
        if jp > 0:
            for d in order:
                a_copy(d, jp - 1, (me_r + d) % rows, me_r).start()

    w_qvg = jnp.concatenate(pair_rows(tr(wq_ref[...]), e) + pair_rows(tr(wv_ref[...]), e) + pair_rows(tr(wg_ref[...]), e), 0)
    k_rows = pair_rows(tr(wk_ref[...]), e)
    k_pad = jnp.zeros((lanes - e2, lanes), BF16)
    w_kh = jnp.concatenate([b for h in range(heads) for b in (k_rows[2 * h], k_rows[2 * h + 1], k_pad)], 0)
    masked = jnp.broadcast_to(mask_ref[...] == 0, (lanes, n))
    lane_row = lax.broadcasted_iota(jnp.int32, (lanes, n), 0)
    fill = jnp.zeros((lanes, n), F32)
    for t, f in enumerate(fill_terms()):
        fill = jnp.where(masked & (lane_row == e2 + t), f, fill)
    fill_col = jnp.transpose(fill)
    row_id = lax.broadcasted_iota(jnp.int32, (e, 2 * tj), 0)
    ones_rows = jnp.where(row_id < 3, 1.0, 0.0).astype(BF16)
    eye_r = lax.broadcasted_iota(jnp.int32, (tj, 2 * tj), 0)
    eye_c = lax.broadcasted_iota(jnp.int32, (tj, 2 * tj), 1)
    eye2 = jnp.where(eye_r == lax.rem(eye_c, tj), 1.0, 0.0).astype(BF16)
    z16 = jnp.zeros((e, tj), BF16)
    z_rows = jnp.zeros((lanes - 3 * e, 2 * tj), BF16)

    for d in order:
        x_copy(d, me_r, (me_r + rows - d) % rows).wait_recv()
    f_copy(0, me_c, mine).start()
    for d in y_order:
        y_copy(d, me_c).start()

    def wait_cols(jp):
        for d in order:
            a_copy(d, jp, me_r, (me_r + rows - d) % rows).wait_recv()

    def project(jp):
        a = a_ref[jp]
        r = mm_nt(w_qvg, a)
        q = (r[:proj2] * q_scale).astype(BF16)
        g = jax.nn.sigmoid(r[2 * proj2:])
        vt[jp] = r[proj2:2 * proj2].astype(BF16)
        for ib in range(cols):
            ls = slice(ib * tj, (ib + 1) * tj)
            gt[jp, ib] = g[:, ls]
            for h in range(heads):
                qp[jp, ib, h, 0:e, 0:tj] = q[h * e2:h * e2 + e, ls]
                qp[jp, ib, h, 0:e, tj:2 * tj] = z16
                qp[jp, ib, h, e:e2, 0:tj] = z16
                qp[jp, ib, h, e:e2, tj:2 * tj] = q[h * e2 + e:h * e2 + e2, ls]
                qp[jp, ib, h, e2:3 * e, :] = ones_rows
        k = mm_nt(a, w_kh)
        for h in range(heads):
            kh[jp, h] = (k[:, h * lanes:(h + 1) * lanes] + fill_col).astype(BF16)

    blk_a, blk_b, blk_d = (me_c + 1) % cols, (me_c + cols - 1) % cols, (me_c + 2) % cols

    halves = 2
    ck = n // halves
    slots = heads

    def scores_dot(ib, jp, h):
        rhs = jnp.concatenate([qp[jp, ib, h], z_rows, eye2], 0)
        return jnp.concatenate([mm(jnp.concatenate([kh[jp, h, c * ck:(c + 1) * ck], bias_ref[ib, h, c * ck:(c + 1) * ck]], 1), rhs) for c in range(halves)], 0)

    def drain(s, c, slot, mx):
        part = s[c * ck:(c + 1) * ck]
        ss[slot, c * ck:(c + 1) * ck] = part
        part = jnp.max(part.reshape(ck // 8, 8, 2 * tj), axis=0)
        return part if mx is None else jnp.maximum(mx, part)

    def weigh(jp, h, slot, c, l, o):
        rs = slice(c * ck, (c + 1) * ck)
        p = jnp.exp(ss[slot, rs] - mm_s[slot])
        part = jnp.sum(p.reshape(ck // 8, 8, 2 * tj), axis=0)
        ob = mm(vt[jp, h * e2:(h + 1) * e2, rs], p.astype(BF16))
        return (part, ob) if l is None else (l + part, o + ob)

    def scores(ib, jp, h):
        s = scores_dot(ib, jp, h)
        mx = None
        for c in range(halves):
            mx = drain(s, c, h, mx)
        mm_s[h] = jnp.max(mx, axis=0, keepdims=True)

    def finish_unit(jp, ib):
        parts = []
        for h in range(heads):
            l1 = jnp.sum(lp[h], axis=0, keepdims=True)
            for half in range(2):
                ls = slice(half * tj, (half + 1) * tj)
                rs = slice(h * e2 + half * e, h * e2 + (half + 1) * e)
                parts.append(gt[jp, ib, rs, :] * (os_[h, half * e:(half + 1) * e, ls] / l1[:, ls]))
        outb[jp, pl.ds(pl.multiple_of(ib * tj, tj), tj), :] = jnp.transpose(jnp.concatenate(parts, 0)).astype(BF16)

    def out_copy(dst_row, jp, count):
        rs, js = pl.ds(pl.multiple_of(dst_row * ti, ti), ti), pl.ds(jp, count)
        return remote(outb.at[js, rs, :], out_ref.at[me_r, js], o_sem.at[0, dst_row], o_sem.at[1, me_r], {'row': dst_row})

    def send_out(jp, ib, count=1):
        for k in range(per_blk):
            dst_row = ib * per_blk + k

            @pl.when(dst_row != me_r)
            def _():
                out_copy(dst_row, jp, count).start()

    def attend(jp, ib, jp_prev, ib_prev, jp_next, ib_next):
        finish_unit(jp_prev, ib_prev)
        for h in range(heads):
            nxt = (ib, jp, h + 2) if h + 2 < heads else (ib_next, jp_next, h + 2 - heads)
            s = scores_dot(*nxt)
            l, o, mx = None, None, None
            for c in range(halves):
                mx = drain(s, c, nxt[2], mx)
                l, o = weigh(jp, h, h, c, l, o)
            mm_s[nxt[2]] = jnp.max(mx, axis=0, keepdims=True)
            os_[h] = o
            lp[h] = l

    os_[...] = jnp.ones_like(os_)
    lp[...] = jnp.ones_like(lp)
    wait_cols(0)
    project(0)
    f_copy(0, me_c, other).wait_recv()
    for h in range(2):
        scores(me_c, 0, h)

    def bring(blk):
        d = (me_c - blk + cols) % cols
        y_copy(d, blk).wait_recv()
        f_copy(d, blk, mine).start()

    def relay(side, blk, step):
        part = pl.ds(core * hh + side * (hh // 2), hh // 2)
        return remote(bias_ref.at[blk, part], bias_ref.at[blk, part], g_sem.at[0, side], g_sem.at[1, side], {'col': (me_c + step) % cols})

    def brought(blk):
        f_copy((me_c - blk + cols) % cols, blk, other).wait_recv()

    def chain(units, prev, nxt):
        seq = [prev] + units + [nxt]
        for k in range(1, len(seq) - 1):
            attend(*seq[k], *seq[k - 1], *seq[k + 1])

    def pick(cond, yes, no):
        return tuple(jnp.where(cond, y, n) for y, n in zip(yes, no))

    n_a = hj // 2

    def lead_in(t, _):
        wait_cols(t + 1)
        project(t + 1)

        @pl.when(t == n_a - 1)
        def _():
            bring(blk_a)
            relay(0, blk_a, cols - 1).start()
            bring(blk_b)
            relay(1, blk_b, 1).start()

        chain([(t, me_c)], (jnp.maximum(t - 1, 0), me_c), (t + 1, me_c))
        return 0

    lax.fori_loop(0, n_a, lead_in, 0)
    brought(blk_a)
    brought(blk_b)

    def role(offsets):
        return (me_c + sum(jnp.where(shift == k, o, 0) for k, o in enumerate(offsets))) % cols

    shift = (chip - me_c + cols) % cols
    odd = chip % 2
    blk_p, blk_q, blk_r = role((1 + 2 * odd, 3, 1, 1)), role((2, 2, 3, 2)), role((3 - 2 * odd, 1, 2, 3))

    def late(w):
        own = shift == 0
        jp = jnp.where(w < 0, w + hj, jnp.where(own, 2 * (w // 4) + w % 2, w % hj))
        second = jnp.where(own, (w // 2) % 2, w // hj)
        return jp, jnp.where(w < 0, blk_p, jnp.where(second == 0, blk_q, blk_r))

    def send_earlier(t):
        k = 2 * (t - n_a)

        @pl.when(t == n_a + 1)
        def _():
            send_out(0, me_c, n_a)

        @pl.when(t > n_a + 1)
        def _():
            send_out(k - 4, blk_p, 2)

    def three(t, _):
        wait_cols(t + 1)
        project(t + 1)
        k = 2 * (t - n_a)
        chain([(t, me_c), (k, blk_p), (k + 1, blk_p)], pick(t == n_a, (t - 1, me_c), (k - 1, blk_p)), (t + 1, me_c))
        return 0

    lax.fori_loop(n_a, hj - 1, three, 0)
    relay(0, blk_d, cols - 1).wait_recv()
    relay(1, blk_d, 1).wait_recv()
    f_copy(2, blk_d, mine).start()

    def bridge(t, _):
        send_out(0, me_c, n_a)
        send_out(0, blk_p, n_a)
        k = 2 * (t - n_a)
        chain([(t, me_c), (k, blk_p), (k + 1, blk_p)], (k - 1, blk_p), (0, blk_q))
        return 0

    brought(blk_d)
    lax.fori_loop(hj - 1, hj, bridge, 0)

    def four(s, _):
        @pl.when(s == 0)
        def _():
            send_out(n_a, me_c, n_a)
            send_out(hj - 4, blk_p, 2)

        @pl.when(s > 0)
        def _():
            send_out(*late(4 * s - 6), 2)
            send_out(*late(4 * s - 4), 2)

        chain([late(4 * s + k) for k in range(4)], late(4 * s - 1), late(jnp.minimum(4 * s + 4, 2 * hj - 1)))
        return 0

    lax.fori_loop(0, hj // 2, four, 0)
    send_out(*late(2 * hj - 6), 2)
    send_out(*late(2 * hj - 4), 2)
    finish_unit(*late(2 * hj - 1))
    send_out(*late(2 * hj - 2), 2)
    own = pltpu.make_async_copy(outb.at[:, my_rows, :], out_ref.at[me_r], l_sem)
    own.start()

    for d in order:
        x_copy(d, (me_r + d) % rows, me_r).wait_send()
        for jp in range(hj):
            a_copy(d, jp, (me_r + d) % rows, me_r).wait_send()
    for d in y_order:
        y_copy(d, me_c).wait_send()
    relay(0, blk_a, cols - 1).wait_send()
    relay(1, blk_b, 1).wait_send()
    for d in range(cols):
        f_copy(d, me_c, mine).wait_send()

    def all_out(send_row, slot):
        rs = pl.ds(pl.multiple_of(send_row * ti, ti), ti)
        return remote(outb.at[:, rs, :], out_ref.at[slot], o_sem.at[0, send_row], o_sem.at[1, slot], {'row': partner})

    for d in order:
        src = (me_r + rows - d) % rows
        all_out(src, src).wait_recv()
    own.wait()
    for d in order:
        dst = (me_r + d) % rows
        all_out(dst, dst).wait_send()


def finish_kernel(e, g_ref, z_ref, wo_ref, out_ref, stage):
    rows, hj, ti, lanes = g_ref.shape
    ch, tj = z_ref.shape[1:]
    pitch = ti + PAD
    n_rj = rows * hj
    wo = wo_ref[...].astype(F32)
    z = jnp.zeros((e, ch), F32)
    wo = tr(jnp.concatenate([blk for r in range(0, wo.shape[0], e) for blk in (wo[r:r + e], z)], 0))
    for rj in range(n_rj):
        stage[rj * pitch:rj * pitch + ti, :] = g_ref[rj // hj, rj % hj].astype(F32)
    def columns(i):
        x = stage[pl.ds(i, n_rj, stride=pitch), :]
        y = pltpu.roll(x, lanes - e, 1)
        return jnp.concatenate([x.reshape(rows, 1, hj, lanes), y.reshape(rows, 1, hj, lanes)], 1).reshape(tj, lanes).astype(BF16)

    for i in range(0, ti, 4):
        r = mm_nt(wo, jnp.concatenate([columns(i + k) for k in range(4)], 0))
        for k in range(4):
            out_ref[i + k] = (r[:, k * tj:(k + 1) * tj] + z_ref[i + k].astype(F32)).astype(BF16)


VM = pl.BlockSpec(memory_space=pltpu.VMEM)


def solution(mesh):
    rows, cols = mesh.shape['row'], mesh.shape['col']

    def body(pair_tile, res_mask, ln_gamma, ln_beta, w_q, w_k, w_v, w_b, w_g, w_o):
        ti, tj, ch = pair_tile.shape
        heads = w_b.shape[1]
        proj = w_q.shape[1]
        n = ti * rows
        hj = tj // rows // 2
        z = jnp.transpose(pair_tile, (0, 2, 1))
        dma = pltpu.SemaphoreType.DMA
        e = proj // heads
        back = pl.pallas_call(
            functools.partial(triangle_kernel, rows, cols),
            out_shape=jax.ShapeDtypeStruct((rows, hj, ti, 2 * ch), BF16),
            in_specs=[VM] * 9,
            out_specs=pl.BlockSpec(memory_space=pl.ANY),
            scratch_shapes=[
                pltpu.VMEM((ti * (rows * hj + PAD), 2 * ch), F32),
                pltpu.VMEM((ti * heads, tj), F32),
                pltpu.VMEM((heads, ti, tj), BF16),
                pltpu.VMEM((rows, hj, ti, 2 * ch), BF16),
                pltpu.VMEM((hj, n, 2 * ch), BF16),
                pltpu.VMEM((cols, heads, n, tj), BF16),
                pltpu.VMEM((hj, cols, heads, 3 * e, 2 * tj), BF16),
                pltpu.VMEM((hj, 2 * proj, n), BF16),
                pltpu.VMEM((hj, cols, 2 * proj, tj), F32),
                pltpu.VMEM((hj, heads, n, 2 * ch), BF16),
                pltpu.VMEM((heads, n, 2 * tj), F32),
                pltpu.VMEM((heads, 1, 2 * tj), F32),
                pltpu.VMEM((heads, 8, 2 * tj), F32),
                pltpu.VMEM((heads, 2 * e, 2 * tj), F32),
                pltpu.VMEM((hj, n, 2 * proj), BF16),
                dma((2, hj, rows)), dma((2, rows)), dma((2, cols)), dma((2, cols)), dma((2, 2)), dma((2, rows)), dma,
            ],
            compiler_params=pltpu.CompilerParams(collective_id=0, has_side_effects=True),
            name='triangle',
        )(z, ln_gamma.reshape(1, ch), ln_beta.reshape(1, ch), w_b.T, res_mask.reshape(1, n), w_q, w_k, w_v, w_g)
        chunk = ti // 2
        out = pl.pallas_call(
            functools.partial(finish_kernel, proj // heads),
            out_shape=jax.ShapeDtypeStruct((ti, ch, tj), BF16),
            grid=(ti // chunk,),
            in_specs=[
                pl.BlockSpec((rows, hj, chunk, 2 * ch), lambda i: (0, 0, i, 0)),
                pl.BlockSpec((chunk, ch, tj), lambda i: (i, 0, 0)),
                pl.BlockSpec((proj, ch), lambda i: (0, 0)),
            ],
            out_specs=pl.BlockSpec((chunk, ch, tj), lambda i: (i, 0, 0)),
            scratch_shapes=[pltpu.VMEM((rows * hj * (chunk + PAD), 2 * ch), F32)],
            name='finish',
        )(back, z, w_o)
        return jnp.transpose(out, (0, 2, 1))

    tile_spec = P(('data', 'row'), 'col', None)
    return jax.shard_map(body, mesh=mesh, in_specs=(tile_spec, P('data'), P(), P(), P(), P(), P(), P(), P(), P()), out_specs=tile_spec, check_vma=False)
```
